32 devices in a mesh: dom: 4 (over y, core), slab: 8 (over z, x).
Axes of the slice: x: 2, y: 2, z: 4, core: 2. Of those that a mesh axis runs over, the one named last changes fastest.
Arguments:
- heat_level: float32 [524288], P(('dom', 'slab')), may hold values from -6 to 6
- emitting_vertex_position: int32 [32, 3, 3, 8192], P(('dom', 'slab')), may hold values from 0 to 16383
- corner_holder_shift: int32 [4, 32, 64, 512], P(None, 'dom', 'slab'), may hold values from 0 to 8, as said below
- corner_fetched_bucket: int32 [4, 32, 64, 512], P(None, 'dom', 'slab'), may hold values from 0 to 8191
- corner_factors: float32 [4, 32, 64, 512], P(None, 'dom', 'slab'), may hold values from 0.05 to 0.5
- diagonal_rigidity: float32 [32, 64, 512], P('dom', 'slab'), may hold values from 0.25 to 2
- boundary_vertex_position: int32 [32, 3, 3, 128], P(('dom', 'slab')), may hold values from 0 to 32767
- boundary_bucket_tally: int32 [32, 9], P(('dom', 'slab')), may hold values from 1 to 128, 576 in all within a row
- boundary_accepting_vertex: int32 [32, 3, 3, 128], P(('dom', 'slab')), may hold values from 0 to 16383
Outputs:
- displacement: float32 [3, 32, 64, 512], P(None, 'dom', 'slab')
- thermal_disp: float32 [3, 524288], P(None, ('dom', 'slab'))
The draws below stay inside these ranges and needn't reach their ends.
Inputs may be any that keep to these rules, and one draw needn't show every extreme that they name: emitting_vertex_position stays below 16384. corner_holder_shift is 3 a + b for an offset (a, b) of the hex node's device that names a device inside the mesh.
All inputs are finite; a program needn't handle non-finite values.
Results may differ from the reference program's by a relative error of at most 0.0001.
Values sent between devices are 32-bit elements; how exact they have to be, the bound alone decides.
No kernel may reach another device: no remote copies, remote signals or barrier semaphores. Data moves between devices by JAX's collectives and lax.ppermute only.
A program may use at most 192 MiB of HBM per device.

```python
import math
import jax
import jax.numpy as jnp
import numpy as np

CX = 8
CY = 8
CZ = 512
HEAT_POINTS_SHARE = 16384
SLOT = 8192
WSLOT = 128
ITERS = 4
NX = 32
NY = 64
NZ = 512
HEAT_MESH_POINTS = 524288
N_DOM = 4
N_SLAB = 8
DEVICES = 32


def draw_corner_holder_shift(key, part):
    dom_total = NX // CX
    slab_total = NY // CY
    coarse_key = jax.random.fold_in(key, 11)
    other_key = jax.random.fold_in(key, 23)
    keep_key = jax.random.fold_in(key, 37)
    coarse = jax.random.randint(coarse_key, (NX, NY, NZ // 8), 0, 9)
    primary = jnp.repeat(coarse, 8, axis=2)
    other = jax.random.randint(other_key, (4, NX, NY, NZ), 0, 9)
    keep = jax.random.randint(keep_key, (4, NX, NY, NZ), 0, 4) < 3
    pick = jnp.where(keep, primary[None], other)
    offset_a = pick // 3
    offset_b = pick % 3
    dom_pos = (jnp.arange(NX, dtype=jnp.int32) // CX)[None, :, None, None]
    slab_pos = (jnp.arange(NY, dtype=jnp.int32) // CY)[None, None, :, None]
    near_dom = dom_pos + offset_a - 1
    near_slab = slab_pos + offset_b - 1
    inside = (near_dom >= 0) & (near_dom < dom_total) & (near_slab >= 0) & (near_slab < slab_total)
    return jnp.where(inside, pick, 4).astype(jnp.int32)


def place_ends(values, stream_key, least, top_value):
    longest = values.shape.index(max(values.shape))
    spots = []
    for shift in (0, 1):
        where = [jax.random.randint(jax.random.fold_in(stream_key, axis), (), 0, length) for axis, length in enumerate(values.shape)]
        where[longest] = (where[longest] + shift) % values.shape[longest]
        spots.append(tuple(where))
    return values.at[spots[0]].set(least).at[spots[1]].set(top_value)


def block_scale(stream_key, shape, split, smallest, top_value):
    factor_of = 1.0
    for position, blocks in split:
        draws = jax.random.uniform(jax.random.fold_in(jax.random.fold_in(stream_key, 6), position), (blocks,), jnp.float32, smallest / len(split), top_value / len(split))
        factor_of = factor_of * jnp.repeat(jnp.exp(draws), shape[position] // blocks).reshape((-1,) + (1,) * (len(shape) - 1 - position))
    return factor_of


def length_profile(amount, total, reach, lean):
    portions = [(1 << 20) // math.isqrt(grade ** lean) + 1 for grade in range(2, amount + 1)]
    spare, holding = total - reach - (amount - 1), [1] * (amount - 1)
    while spare > 0:
        movable = [i for i in range(amount - 1) if holding[i] < reach]
        whole, left = sum([portions[i] for i in movable]), spare
        for i in movable:
            more = min(reach - holding[i], max(1, left * portions[i] // whole), spare)
            holding[i] = holding[i] + more
            spare = spare - more
    return np.array([reach] + holding)


def ragged(own_key, count, total, bound, slope):
    if count == 2:
        one = jax.random.randint(own_key, (), max(1, total - bound), min(bound, total - 1) + 1)
        return jnp.stack([one, total - one])
    tallies = jnp.asarray(length_profile(count, total, bound, slope), jnp.int32)
    couples = (count - 1) // 2
    giver, taker = tallies[1:1 + 2 * couples:2], tallies[2:2 + 2 * couples:2]
    room = jnp.minimum(giver - 1, bound - taker)
    moved = jax.random.randint(jax.random.fold_in(own_key, 1), (couples,), 0, 1 << 20) % (room + 1)
    tallies = tallies.at[1:1 + 2 * couples:2].set(giver - moved).at[2:2 + 2 * couples:2].set(taker + moved)
    return tallies[jax.random.permutation(jax.random.fold_in(own_key, 2), count)]


def noise(key, dims, spread, limit, cuts=(), kind=jnp.bfloat16):
    level = block_scale(key, dims, cuts, -0.22, 0.18) if cuts else 1.0
    array = jax.random.normal(key, dims, jnp.float32) * spread * level
    return jnp.minimum(jnp.maximum(array, -limit), limit).astype(kind)


def setup_inputs(seed: int = 0) -> dict:
    key_of = jax.random.split(jax.random.key(seed), 10)
    return {
        "heat_level": noise(key_of[0], (HEAT_MESH_POINTS,), 1.0, 6.0, ((0, 32),), jnp.float32),
        "emitting_vertex_position": place_ends(jax.random.randint(key_of[1], (DEVICES, 3, 3, SLOT), 0, min(HEAT_POINTS_SHARE, 65280)), jax.random.fold_in(key_of[1], 1), 0, (min(HEAT_POINTS_SHARE, 65280)) - 1).astype(jnp.int32),
        "corner_holder_shift": draw_corner_holder_shift(jax.random.fold_in(key_of[9], 71), 0),
        "corner_fetched_bucket": place_ends(jax.random.randint(key_of[3], (4, NX, NY, NZ), 0, SLOT), jax.random.fold_in(key_of[3], 1), 0, SLOT - 1).astype(jnp.int32),
        "corner_factors": jnp.clip(0.05 + 0.45 * jax.random.uniform(key_of[4], (4, NX, NY, NZ), jnp.float32) ** block_scale(key_of[4], (4, NX, NY, NZ), ((1, 4), (2, 8)), -0.2, 0.2), 0.05, 0.5),
        "diagonal_rigidity": jnp.clip(0.25 + 1.75 * jax.random.uniform(key_of[5], (NX, NY, NZ), jnp.float32) ** block_scale(key_of[5], (NX, NY, NZ), ((0, 4), (1, 8)), -0.2, 0.2), 0.25, 2.0),
        "boundary_vertex_position": place_ends(jax.random.randint(key_of[6], (DEVICES, 3, 3, WSLOT), 0, CX * CY * CZ), jax.random.fold_in(key_of[6], 1), 0, (CX * CY * CZ) - 1).astype(jnp.int32),
        "boundary_bucket_tally": jax.vmap(lambda own: ragged(own, 9, 9 * WSLOT // 2, WSLOT, 2))(jax.random.split(key_of[7], DEVICES)).reshape((DEVICES, 9)).astype(jnp.int32),
        "boundary_accepting_vertex": place_ends(jax.random.randint(key_of[8], (DEVICES, 3, 3, WSLOT), 0, HEAT_POINTS_SHARE), jax.random.fold_in(key_of[8], 1), 0, HEAT_POINTS_SHARE - 1).astype(jnp.int32),
    }


COEF = 0.5


def operate(bucket_entries, diagonal_rigidity):
    padded = jnp.pad(bucket_entries, ((0, 0), (1, 1), (1, 1), (1, 1)))
    beside = padded[:, 2:, 1:-1, 1:-1] + padded[:, :-2, 1:-1, 1:-1]
    beside = beside + padded[:, 1:-1, 2:, 1:-1] + padded[:, 1:-1, :-2, 1:-1]
    beside = beside + padded[:, 1:-1, 1:-1, 2:] + padded[:, 1:-1, 1:-1, :-2]
    return (6.0 + diagonal_rigidity)[None] * bucket_entries - beside


def neighbour(dom_of, slab_of, offset_a, offset_b):
    near_dom = dom_of + offset_a - 1
    near_slab = slab_of + offset_b - 1
    inside = (near_dom >= 0) & (near_dom < N_DOM) & (near_slab >= 0) & (near_slab < N_SLAB)
    providing_holder = jnp.clip(near_dom, 0, N_DOM - 1) * N_SLAB + jnp.clip(near_slab, 0, N_SLAB - 1)
    return inside, providing_holder.astype(jnp.int32)


def reference(heat_level, emitting_vertex_position, corner_holder_shift, corner_fetched_bucket, corner_factors, diagonal_rigidity, boundary_vertex_position, boundary_bucket_tally, boundary_accepting_vertex):
    devices = N_DOM * N_SLAB
    dev_ids = jnp.arange(devices, dtype=jnp.int32)
    dom_of = dev_ids // N_SLAB
    slab_of = dev_ids % N_SLAB
    pieces = []
    for offset_a in range(3):
        for offset_b in range(3):
            inside, providing_holder = neighbour(dom_of, slab_of, offset_a, offset_b)
            device_portion = emitting_vertex_position[providing_holder, 2 - offset_a, 2 - offset_b]
            bucket_entries = heat_level[providing_holder[:, None] * HEAT_POINTS_SHARE + device_portion]
            pieces.append(jnp.where(inside[:, None], bucket_entries, jnp.zeros_like(bucket_entries)))
    received = jnp.stack(pieces, 1).reshape(devices, 9 * SLOT)
    owner_rows = (jnp.arange(NX, dtype=jnp.int32) // CX) * N_SLAB
    owner_map = owner_rows[:, None] + (jnp.arange(NY, dtype=jnp.int32) // CY)[None, :]
    interp = jnp.zeros((NX, NY, NZ), jnp.float32)
    for corner in range(4):
        column = corner_holder_shift[corner] * SLOT + corner_fetched_bucket[corner]
        interp = interp + corner_factors[corner] * received[owner_map[:, :, None], column]
    padded = jnp.pad(interp, 1)
    thermal_load = COEF * jnp.stack([
        padded[2:, 1:-1, 1:-1] - padded[:-2, 1:-1, 1:-1],
        padded[1:-1, 2:, 1:-1] - padded[1:-1, :-2, 1:-1],
        padded[1:-1, 1:-1, 2:] - padded[1:-1, 1:-1, :-2]])
    solution = jnp.zeros_like(thermal_load)
    residual = thermal_load
    direction = thermal_load
    norm_now = jnp.sum(residual * residual)
    for iteration in range(ITERS):
        applied = operate(direction, diagonal_rigidity)
        step_size = norm_now / jnp.sum(direction * applied)
        solution = solution + step_size * direction
        residual = residual - step_size * applied
        norm_next = jnp.sum(residual * residual)
        direction = residual + (norm_next / norm_now) * direction
        norm_now = norm_next
    src_ids = dev_ids[:, None, None, None]
    rows_x = (src_ids // N_SLAB) * CX + boundary_vertex_position // (CY * CZ)
    rows_y = (src_ids % N_SLAB) * CY + (boundary_vertex_position // CZ) % CY
    rows_z = boundary_vertex_position % CZ
    surface = solution[:, rows_x, rows_y, rows_z]
    live = jnp.arange(WSLOT, dtype=jnp.int32)[None, None, None, :] < boundary_bucket_tally.reshape(devices, 3, 3)[:, :, :, None]
    surface = jnp.where(live[None], surface, jnp.zeros_like(surface))
    thermal_disp = jnp.zeros((3, HEAT_MESH_POINTS), jnp.float32)
    for offset_a in range(3):
        for offset_b in range(3):
            inside, providing_holder = neighbour(dom_of, slab_of, offset_a, offset_b)
            bucket_entries = surface[:, providing_holder, 2 - offset_a, 2 - offset_b, :]
            bucket_entries = jnp.where(inside[None, :, None], bucket_entries, jnp.zeros_like(bucket_entries))
            targets = dev_ids[:, None] * HEAT_POINTS_SHARE + boundary_accepting_vertex[:, offset_a, offset_b, :]
            thermal_disp = thermal_disp.at[:, targets.reshape(-1)].add(bucket_entries.reshape(3, -1))
    return solution, thermal_disp
```

```python
import functools
import math

import jax
import jax.numpy as jnp
from jax import lax
from jax.experimental import pallas as pl
from jax.experimental.pallas import tpu as pltpu
from jax.sharding import PartitionSpec as P

ITERS = 4
COEF = 0.5
LANES = 128
SUB = 8
CENTRE = 7.125
HALF = 6.875
REACH = ITERS + 1
VMEM = pl.BlockSpec(memory_space=pltpu.VMEM)
SMEM = pl.BlockSpec(memory_space=pltpu.SMEM)


def params(mib):
    return pltpu.CompilerParams(vmem_limit_bytes=mib * 1024 * 1024)


def lookup(table, first, rows, lanes, bits):
    if rows == 1:
        row = jnp.broadcast_to(table[pl.ds(first, 1), :], lanes.shape)
        return jnp.take_along_axis(row, lanes, axis=1, mode="promise_in_bounds")
    half = rows // 2
    lower = lookup(table, first, half, lanes, bits[:-1])
    upper = lookup(table, first + half, half, lanes, bits[:-1])
    return jnp.where(bits[-1], upper, lower)


def lookup_all(table, indices, chunk):
    rows = table.shape[0]
    depth = int(math.log2(chunk))
    lanes = [index & (LANES - 1) for index in indices]
    high = [index >> 7 for index in indices]
    outer = [value >> depth for value in high]

    def step(block, found):
        base = pl.multiple_of(block * chunk, chunk)
        fresh = []
        for lane, value, top, old in zip(lanes, high, outer, found):
            bits = [((value >> bit) & 1) == 1 for bit in range(depth)]
            fresh.append(jnp.where(top == block, lookup(table, base, chunk, lane, bits), old))
        return tuple(fresh)

    zero = jnp.zeros(indices[0].shape, jnp.float32)
    return lax.fori_loop(0, rows // chunk, step, tuple(zero for _ in indices))


def depart_kernel(heat, picks, out, index):
    ways = picks.shape[1]
    slots = picks.shape[3]
    per = slots // LANES
    for a in range(ways):
        for b in range(ways):
            for row in range(0, per, SUB):
                piece = picks[0, a, b, pl.ds(row * LANES, SUB * LANES)]
                index[pl.ds((a * ways + b) * per + row, SUB), :] = piece.reshape(SUB, LANES)
    group = SUB * SUB

    def body(g, carry):
        base = pl.multiple_of(g * group, group)
        found = lookup_all(heat, [index[pl.ds(base + SUB * k, SUB), :] for k in range(SUB)], 64)
        for k in range(SUB):
            out[pl.ds(base + SUB * k, SUB), :] = found[k]
        return carry

    lax.fori_loop(0, ways * ways * per // group, body, 0)


def interp_kernel(low, near_low, near, near_high, high, shift, bucket, factor, out, table):
    corners, nx, _, nz = shift.shape
    per = near.shape[1]
    slots = per * LANES
    for b, ref in ((0, low), (2, high)):
        for a in range(3):
            table[pl.ds((3 * a + b) * per, per), :] = ref[a]
    for a, ref in enumerate((near_low, near, near_high)):
        table[pl.ds((3 * a + 1) * per, per), :] = ref[1]

    def body(x, carry):
        for z in range(0, nz, 2 * LANES):
            where = []
            for c in range(corners):
                for part in range(2):
                    at = pl.ds(z + part * LANES, LANES)
                    where.append(shift[c, x, :, at] * slots + bucket[c, x, :, at])
            found = lookup_all(table, where, 64)
            for part in range(2):
                at = pl.ds(z + part * LANES, LANES)
                total = factor[0, x, :, at] * found[part]
                for c in range(1, corners):
                    total = total + factor[c, x, :, at] * found[2 * c + part]
                out[x, :, at] = total
        return carry

    lax.fori_loop(0, nx, body, 0)


def pack_kernel(width, low, own, high, up, down):
    ny, nz = own.shape[1:]
    extent = low.shape[0] + own.shape[0] + high.shape[0]
    for t in range(nz // LANES):
        at = pl.ds(t * LANES, LANES)
        for x in range(extent):
            ref, k = low, x
            if k >= low.shape[0]:
                ref, k = own, k - low.shape[0]
                if k >= own.shape[0]:
                    ref, k = high, k - own.shape[0]
            to = pl.ds((t * extent + x) * width, width)
            up[to, :] = ref[k, pl.ds(ny - width, width), at]
            down[to, :] = ref[k, pl.ds(0, width), at]


def unpack(target, margin, width, own, dom_low, dom_high, slab_low, slab_high, change):
    nx, ny, nz = own.shape
    tiles = nz // LANES
    extent = nx + 2 * width
    start = REACH - width
    for t in range(tiles):
        at = pl.ds(t * LANES, LANES)
        for x in range(extent):
            if x < width:
                ref, k = dom_low, x
            elif x < width + nx:
                ref, k = own, x - width
            else:
                ref, k = dom_high, x - width - nx
            rows = pl.ds((t * extent + x) * width, width)
            target[t, start + x, pl.ds(SUB, ny), :] = change(ref[k, :, at], start + x, 1)
            target[t, start + x, pl.ds(SUB - width, width), :] = change(slab_low[rows, :], start + x, 0)
            target[t, start + x, pl.ds(SUB + ny, width), :] = change(slab_high[rows, :], start + x, 2)


def krylov_kernel(inside, own, p_low, p_high, p_left, p_right, rigid, d_low, d_high, d_left, d_right,
                  basis, sums, temp, diag, u0, u1, u2, u3):
    nx, ny, nz = own.shape
    tiles = nz // LANES
    parts = temp.shape[2] // SUB
    held = (u0, u1, u2, u3)
    flag = [inside[k].astype(jnp.float32) for k in range(4)]

    def mask(x, part):
        at_x = jnp.where(x < REACH, flag[0], jnp.where(x >= REACH + nx, flag[1], 1.0))
        return at_x * (flag[2] if part == 0 else flag[3] if part == 2 else 1.0)

    temp[...] = jnp.zeros_like(temp)
    unpack(temp, REACH, REACH, own, p_low, p_high, p_left, p_right, lambda v, x, part: v)
    diag[...] = jnp.zeros_like(diag)
    unpack(diag, REACH, REACH - 2, rigid, d_low, d_high, d_left, d_right,
           lambda v, x, part: (v * (2.0 / HALF) + 2.0 * (6.0 - CENTRE) / HALF) * mask(x, part))
    lane = lax.broadcasted_iota(jnp.int32, (SUB, LANES), 1)
    first, last = lane == 0, lane == LANES - 1
    zero = jnp.zeros((SUB, LANES), jnp.float32)

    def around_z(values):
        back = [pltpu.roll(v, 1, axis=1) for v in values]
        ahead = [pltpu.roll(v, LANES - 1, axis=1) for v in values]
        pairs = []
        for t in range(tiles):
            before = jnp.where(first, back[t - 1] if t else zero, back[t])
            after = jnp.where(last, ahead[t + 1] if t + 1 < tiles else zero, ahead[t])
            pairs.append((before, after))
        return pairs

    def around_y(ref, head, x, part):
        base = part * SUB
        mine = ref[(*head, x, pl.ds(base, SUB))]
        below = pltpu.roll(mine, 1, axis=0) if part == 0 else ref[(*head, x, pl.ds(base - 1, SUB))]
        above = pltpu.roll(mine, SUB - 1, axis=0) if part == parts - 1 else ref[(*head, x, pl.ds(base + 1, SUB))]
        return mine, below, above

    def load_row(x, carry):
        for part in range(parts):
            scale = COEF * mask(x, part)
            rows = [around_y(temp, (t,), x, part) for t in range(tiles)]
            along = around_z([r[0] for r in rows])
            for t in range(tiles):
                ahead = temp[t, x + 1, pl.ds(part * SUB, SUB), :]
                back = temp[t, x - 1, pl.ds(part * SUB, SUB), :]
                u0[0, t, x, pl.ds(part * SUB, SUB), :] = scale * (ahead - back)
                u0[1, t, x, pl.ds(part * SUB, SUB), :] = scale * (rows[t][2] - rows[t][1])
                u0[2, t, x, pl.ds(part * SUB, SUB), :] = scale * (along[t][1] - along[t][0])
        return carry

    lax.fori_loop(1, nx + 2 * REACH - 1, load_row, 0)

    def twice(ref, c, x, part):
        coefficient = (2.0 / HALF) * mask(x, part)
        rows = [around_y(ref, (c, t), x, part) for t in range(tiles)]
        along = around_z([r[0] for r in rows])
        results = []
        for t in range(tiles):
            near = rows[t][1] + rows[t][2] + along[t][0] + along[t][1]
            near = near + ref[c, t, x + 1, pl.ds(part * SUB, SUB), :] + ref[c, t, x - 1, pl.ds(part * SUB, SUB), :]
            results.append(diag[t, x, pl.ds(part * SUB, SUB), :] * rows[t][0] - coefficient * near)
        return results, [r[0] for r in rows]

    for order in range(1, ITERS):
        source, target = held[order - 1], held[order]

        def apply_row(x, carry):
            for c in range(3):
                for part in range(parts):
                    doubled, _ = twice(source, c, x, part)
                    for t in range(tiles):
                        at = (c, t, x, pl.ds(part * SUB, SUB))
                        if order == 1:
                            target[at] = 0.5 * doubled[t]
                        else:
                            target[at] = doubled[t] - held[order - 2][at]
            return carry

        margin = ITERS - order
        lax.fori_loop(REACH - margin, REACH + nx + margin, apply_row, 0)

    def dots_row(x, carry):
        carry = list(carry)
        for c in range(3):
            doubled, u = twice(u3, c, REACH + x, 1)
            for t in range(tiles):
                at = (c, t, REACH + x, pl.ds(SUB, SUB))
                v = [u0[at], u1[at], u2[at], u[t]]
                pairs = [(v[0], v[0]), (v[0], v[1]), (v[1], v[1]), (v[1], v[2]), (v[2], v[2]), (v[2], v[3]),
                         (v[3], v[3]), (v[3], doubled[t])]
                for k, (left, right) in enumerate(pairs):
                    carry[k] = carry[k] + left * right
                for j in range(4):
                    basis[3 * j + c, pl.ds(pl.multiple_of(t * nx * SUB + x * SUB, SUB), SUB), :] = v[j]
        return tuple(carry)

    totals = lax.fori_loop(0, nx, dots_row, tuple(zero for _ in range(8)))
    for k in range(8):
        sums[pl.ds(k, 1), :] = jnp.sum(totals[k], axis=0, keepdims=True)


def surface_kernel(nz, tally, basis, picks, out, index, live):
    fields, rows, _ = basis.shape
    ways = picks.shape[1]
    count = ways * ways
    block = rows // (nz // LANES)
    lane = lax.broadcasted_iota(jnp.int32, (1, LANES), 1)
    index[...] = jnp.zeros_like(index)
    live[...] = jnp.zeros_like(live)
    for a in range(ways):
        for b in range(ways):
            spot = picks[0, a, pl.ds(b, 1), :]
            along = spot % nz
            high = (along // LANES) * block + spot // nz
            index[pl.ds(a * ways + b, 1), :] = high * LANES + spot % LANES
            live[pl.ds(a * ways + b, 1), :] = (lane < tally[0, a * ways + b]).astype(jnp.float32)

    def body(f, carry):
        found = lookup_all(basis.at[f], [index[pl.ds(0, SUB), :], index[pl.ds(SUB, SUB), :]], 64)
        for k in range(count):
            value = found[k // SUB][k % SUB : k % SUB + 1, :]
            value = jnp.where(live[pl.ds(k, 1), :] > 0.5, value, 0.0)
            out[k // ways, k % ways, pl.ds(f, 1), :] = value
        return carry

    lax.fori_loop(0, fields, body, 0)


def coefficients(nu):
    half = 0.5

    def gram(i, j):
        return half * (nu[i + j] + nu[abs(i - j)])

    def inner(i, j):
        if j == 0:
            return gram(i, 1)
        return half * (gram(i, j + 1) + gram(i, j - 1))

    def form(vector, matrix):
        n = len(vector)
        total = None
        for i in range(n):
            for j in range(i, n):
                term = vector[i] * vector[j] * matrix(i, j)
                term = term if i == j else 2.0 * term
                total = term if total is None else total + term
        return total

    one = jnp.ones_like(nu[0])
    found, residual, direction = [], [one], [one]
    rr = nu[0]
    for iteration in range(ITERS):
        energy = form(direction, lambda i, j: CENTRE * gram(i, j) + HALF * inner(i, j))
        alpha = rr / energy
        found = [
            (found[i] if i < len(found) else 0.0) + alpha * direction[i] for i in range(len(direction))
        ]
        if iteration + 1 == ITERS:
            break
        image = [CENTRE * d for d in direction] + [jnp.zeros_like(one)]
        for j, d in enumerate(direction):
            if j == 0:
                image[1] = image[1] + HALF * d
            else:
                image[j + 1] = image[j + 1] + half * HALF * d
                image[j - 1] = image[j - 1] + half * HALF * d
        residual = residual + [jnp.zeros_like(one)]
        residual = [r - alpha * w for r, w in zip(residual, image)]
        fresh = form(residual, gram)
        ratio = fresh / rr
        direction = direction + [jnp.zeros_like(one)]
        direction = [r + ratio * d for r, d in zip(residual, direction)]
        rr = fresh
    return found


def finish_kernel(sums, basis, surface, picks, disp, thermal, shift):
    raw = [jnp.broadcast_to(jnp.sum(sums[pl.ds(k, 1), :], axis=1, keepdims=True), (1, LANES)) for k in range(8)]
    nu = [raw[0], raw[1]]
    for k in range(2, 7):
        nu.append(2.0 * raw[k] - raw[k % 2])
    nu.append(2.0 * raw[7] - nu[5] - 2.0 * raw[1])
    weights = coefficients(nu)
    wide = [jnp.broadcast_to(w, (SUB, LANES)) for w in weights]
    _, nx, ny, nz = disp.shape
    tiles = nz // LANES

    def row(x, carry):
        for c in range(3):
            for t in range(tiles):
                at = pl.ds(pl.multiple_of(t * nx * SUB + x * SUB, SUB), SUB)
                total = wide[0] * basis[c, at, :]
                for j in range(1, 4):
                    total = total + wide[j] * basis[3 * j + c, at, :]
                disp[c, x, :, pl.ds(t * LANES, LANES)] = total
        return carry

    lax.fori_loop(0, nx, row, 0)
    ways = picks.shape[1]
    depth = thermal.shape[1] // LANES
    place = lax.broadcasted_iota(jnp.int32, (LANES, LANES), 0)
    tall = lax.broadcasted_iota(jnp.int32, (depth, LANES), 0)
    total = jnp.zeros((9 * depth, LANES), jnp.float32)
    for a in range(ways):
        for b in range(ways):
            spot = picks[0, a, pl.ds(b, 1), :]
            lane_hot = (place == spot % LANES).astype(jnp.float32).astype(jnp.bfloat16)
            row_hot = tall == spot // LANES
            pieces = []
            for c in range(3):
                value = weights[0] * surface[a, b, pl.ds(c, 1), :]
                for j in range(1, 4):
                    value = value + weights[j] * surface[a, b, pl.ds(3 * j + c, 1), :]
                for _ in range(3):
                    part = value.astype(jnp.bfloat16).astype(jnp.float32)
                    value = value - part
                    pieces.append(jnp.where(row_hot, jnp.broadcast_to(part, row_hot.shape), 0.0))
            left = jnp.concatenate(pieces, axis=0).astype(jnp.bfloat16)
            total = total + lax.dot_general(left, lane_hot, (((1,), (1,)), ((), ())),
                                            preferred_element_type=jnp.float32)
    for c in range(3):
        whole = total[3 * c * depth : (3 * c + 1) * depth]
        whole = whole + total[(3 * c + 1) * depth : (3 * c + 2) * depth]
        shift[...] = whole + total[(3 * c + 2) * depth : (3 * c + 3) * depth]
        for r in range(depth):
            thermal[pl.ds(c, 1), pl.ds(r * LANES, LANES)] = shift[pl.ds(r, 1), :]


def swap(last, leading, axis):
    peers = lax.axis_size(axis)
    up = [(i, i + 1) for i in range(peers - 1)]
    down = [(j, i) for i, j in up]
    return lax.ppermute(last, axis, up), lax.ppermute(leading, axis, down)


def total_over(value, axis):
    peers = lax.axis_size(axis)
    hop = 1
    while hop < peers:
        value = value + lax.ppermute(value, axis, [(i, i ^ hop) for i in range(peers)])
        hop *= 2
    return value


def on_device(heat_level, emitting, holder, bucket, factors, rigidity, boundary, tally, accepting):
    f32 = jnp.float32
    ways = emitting.shape[1]
    slots = emitting.shape[3]
    per = slots // LANES
    nx, ny, nz = rigidity.shape
    tiles = nz // LANES
    call = pl.pallas_call
    heat = heat_level.reshape(-1, LANES)
    departing = call(
        depart_kernel,
        out_shape=jax.ShapeDtypeStruct((ways * ways * per, LANES), f32),
        in_specs=[VMEM] * 2,
        out_specs=VMEM,
        scratch_shapes=[pltpu.VMEM((ways * ways * per, LANES), jnp.int32)],
        name="depart",
    )(heat, emitting).reshape(ways, ways, per, LANES)
    from_low, from_high = swap(departing[2], departing[0], "dom")
    near = departing[1]
    up = jnp.stack([from_low[2], near[2], from_high[2]])
    down = jnp.stack([from_low[0], near[0], from_high[0]])
    left, right = swap(up, down, "slab")

    narrow = REACH - 2

    def packed(width, low, own, high):
        shape = jax.ShapeDtypeStruct((tiles * (nx + 2 * width) * width, LANES), f32)
        return call(functools.partial(pack_kernel, width), out_shape=(shape, shape), in_specs=[VMEM] * 3,
                    out_specs=(VMEM, VMEM), name=f"pack{width}")(low, own, high)

    d_low, d_high = swap(rigidity[nx - narrow :], rigidity[:narrow], "dom")
    d_up, d_down = packed(narrow, d_low, rigidity, d_high)
    d_left, d_right = swap(d_up, d_down, "slab")

    interp = call(
        interp_kernel,
        out_shape=jax.ShapeDtypeStruct((nx, ny, nz), f32),
        in_specs=[VMEM] * 8,
        out_specs=VMEM,
        scratch_shapes=[pltpu.VMEM((ways * ways * per, LANES), f32)],
        compiler_params=params(32),
        name="interp",
    )(left, from_low, near, from_high, right, holder, bucket, factors)

    p_low, p_high = swap(interp[nx - REACH :], interp[:REACH], "dom")
    p_up, p_down = packed(REACH, p_low, interp, p_high)
    p_left, p_right = swap(p_up, p_down, "slab")
    dom, slab = lax.axis_index("dom"), lax.axis_index("slab")
    inside = jnp.stack([dom > 0, dom < lax.axis_size("dom") - 1, slab > 0, slab < lax.axis_size("slab") - 1])
    extent = nx + 2 * REACH
    field = pltpu.VMEM((3, tiles, extent, 3 * SUB, LANES), f32)
    basis, sums = call(
        krylov_kernel,
        out_shape=(jax.ShapeDtypeStruct((3 * ITERS, tiles * nx * ny, LANES), f32), jax.ShapeDtypeStruct((SUB, LANES), f32)),
        in_specs=[SMEM] + [VMEM] * 10,
        out_specs=(VMEM, VMEM),
        scratch_shapes=[pltpu.VMEM((tiles, extent, 3 * SUB, LANES), f32)] * 2 + [field] * 4,
        compiler_params=params(48),
        name="krylov",
    )(inside.astype(jnp.int32), interp, p_low, p_high, p_left, p_right, rigidity, d_low, d_high, d_left, d_right)
    sums = total_over(total_over(sums, "dom"), "slab")
    surface = call(
        functools.partial(surface_kernel, nz),
        out_shape=jax.ShapeDtypeStruct((ways, ways, 3 * ITERS, LANES), f32),
        in_specs=[SMEM, VMEM, VMEM],
        out_specs=VMEM,
        scratch_shapes=[pltpu.VMEM((2 * SUB, LANES), jnp.int32), pltpu.VMEM((2 * SUB, LANES), f32)],
        compiler_params=params(16),
        name="surface",
    )(tally, basis, boundary)
    s_low, s_high = swap(surface[2], surface[0], "dom")
    stacked = jnp.stack([s_low, surface[1], s_high])
    s_left, s_right = swap(stacked[:, 2], stacked[:, 0], "slab")
    arrived = jnp.stack([s_left, stacked[:, 1], s_right], axis=1)
    return call(
        finish_kernel,
        out_shape=(jax.ShapeDtypeStruct((3, nx, ny, nz), f32), jax.ShapeDtypeStruct((3, heat_level.shape[0]), f32)),
        in_specs=[VMEM] * 4,
        out_specs=(VMEM, VMEM),
        scratch_shapes=[pltpu.VMEM((heat_level.shape[0] // LANES, LANES), f32)],
        compiler_params=params(32),
        name="finish",
    )(sums, basis, arrived, accepting)


def solution(mesh):
    both = ("dom", "slab")
    in_specs = (
        P(both),
        P(both, None, None, None),
        P(None, "dom", "slab", None),
        P(None, "dom", "slab", None),
        P(None, "dom", "slab", None),
        P("dom", "slab", None),
        P(both, None, None, None),
        P(both, None),
        P(both, None, None, None),
    )
    out_specs = (P(None, "dom", "slab", None), P(None, both))
    return jax.shard_map(on_device, mesh=mesh, in_specs=in_specs, out_specs=out_specs, check_vma=False)
```

```python
import functools
import math

import jax
import jax.numpy as jnp
from jax import lax
from jax.experimental import pallas as pl
from jax.experimental.pallas import tpu as pltpu
from jax.sharding import PartitionSpec as P

ITERS = 4
COEF = 0.5
LANES = 128
CHUNK = 16
WEIGHT = 4e8
SUB = 8
CENTRE = 7.125
HALF = 6.875
REACH = ITERS + 1
VMEM = pl.BlockSpec(memory_space=pltpu.VMEM)
SMEM = pl.BlockSpec(memory_space=pltpu.SMEM)


def params(mib):
    return pltpu.CompilerParams(vmem_limit_bytes=mib * 1024 * 1024)


def cost(micro, moved=0):
    return pl.CostEstimate(flops=int(micro * WEIGHT), bytes_accessed=moved, transcendentals=0)


def lookup(table, first, rows, lanes, bits):
    if rows == 1:
        row = jnp.broadcast_to(table[pl.ds(first, 1), :], lanes.shape)
        return jnp.take_along_axis(row, lanes, axis=1, mode="promise_in_bounds")
    half = rows // 2
    lower = lookup(table, first, half, lanes, bits[:-1])
    upper = lookup(table, first + half, half, lanes, bits[:-1])
    return jnp.where(bits[-1], upper, lower)


def lookup_all(table, indices, chunk):
    rows = table.shape[0]
    depth = int(math.log2(chunk))
    lanes = [index & (LANES - 1) for index in indices]
    high = [index >> 7 for index in indices]
    outer = [value >> depth for value in high]

    def step(block, found):
        base = pl.multiple_of(block * chunk, chunk)
        fresh = []
        for lane, value, top, old in zip(lanes, high, outer, found):
            bits = [((value >> bit) & 1) == 1 for bit in range(depth)]
            fresh.append(jnp.where(top == block, lookup(table, base, chunk, lane, bits), old))
        return tuple(fresh)

    zero = jnp.zeros(indices[0].shape, jnp.float32)
    return lax.fori_loop(0, rows // chunk, step, tuple(zero for _ in indices))


def order2(a, b):
    if len(a) == 1:
        return (jnp.minimum(a[0], b[0]),), (jnp.maximum(a[0], b[0]),)
    swap = a[0] > b[0]
    low = [jnp.minimum(a[0], b[0])] + [jnp.where(swap, y, x) for x, y in zip(a[1:], b[1:])]
    high = [jnp.maximum(a[0], b[0])] + [jnp.where(swap, x, y) for x, y in zip(a[1:], b[1:])]
    return tuple(low), tuple(high)

def sublane_xor(value, mask):
    sub = lax.broadcasted_iota(jnp.int32, value.shape, 0)
    return jnp.take_along_axis(value, sub ^ mask, axis=0, mode="promise_in_bounds")

def keep_one(a, other, lower):
    if len(a) == 1:
        return (jnp.where(lower, jnp.minimum(a[0], other[0]), jnp.maximum(a[0], other[0])),)
    take = (a[0] > other[0]) == lower
    return tuple(jnp.where(take, y, x) for x, y in zip(a, other))

def sort_rows(refs, block):
    count = refs[0].shape[0] // SUB
    def load(v):
        at = pl.ds(pl.multiple_of(v * SUB, SUB), SUB)
        return tuple(r[at, :] for r in refs)
    def store(v, value):
        at = pl.ds(pl.multiple_of(v * SUB, SUB), SUB)
        for r, x in zip(refs, value): r[at, :] = x
    def strides(held, stride):
        while stride:
            for i in range(len(held)):
                if not i & stride:
                    held[i], held[i | stride] = order2(held[i], held[i | stride])
            stride //= 2
    def whole(t, carry):
        held = [load(t * block + i) for i in range(block)]
        size = 2
        while size <= block:
            for i in range(block):
                j = i ^ (size - 1)
                if i < j: held[i], held[j] = order2(held[i], held[j])
            strides(held, size // 4)
            size *= 2
        for i in range(block): store(t * block + i, held[i])
        return carry
    def finish(t, carry):
        held = [load(t * block + i) for i in range(block)]
        strides(held, block // 2)
        for i in range(block): store(t * block + i, held[i])
        return carry
    lax.fori_loop(0, count // block, whole, 0)
    size = 2 * block
    while size <= count * SUB:
        span = min(size, count)
        flip = size // count - 1 if size > count else 0
        groups = span // block
        def top(t, carry):
            base = (t // (block // 2)) * span
            i = t % (block // 2)
            spots = []
            for j in range(groups):
                spots += [base + i + block * j, base + block - 1 - i + block * j]
            held = [load(v) for v in spots]
            n = len(held)
            if flip:
                sub = lax.broadcasted_iota(jnp.int32, (SUB, LANES), 0)
                lower = (sub & ((flip + 1) // 2)) == 0
                turned = [tuple(sublane_xor(x, flip) for x in h) for h in held]
                held = [keep_one(held[k], turned[n - 1 - k], lower) for k in range(n)]
                bit = (flip + 1) // 4
                while bit:
                    lower = (sub & bit) == 0
                    held = [keep_one(h, tuple(sublane_xor(x, bit) for x in h), lower) for h in held]
                    bit //= 2
                far = groups // 2
            else:
                for k in range(n // 2):
                    held[k], held[n - 1 - k] = order2(held[k], held[n - 1 - k])
                far = groups // 4
            while far:
                for j in range(groups):
                    if not j & far:
                        for side in range(2):
                            x, y = 2 * j + side, 2 * (j | far) + side
                            held[x], held[y] = order2(held[x], held[y])
                far //= 2
            for v, h in zip(spots, held): store(v, h)
            return carry
        lax.fori_loop(0, (count // span) * (block // 2), top, 0)
        lax.fori_loop(0, count // block, finish, 0)
        size *= 2


def plan_kernel(per, rows, shift, bucket, keys, bounds):
    corners, nx, _, nz = shift.shape
    tiles = nz // LANES
    count = corners * nx * tiles
    sub = lax.broadcasted_iota(jnp.int32, (SUB, LANES), 0)
    def build(x, carry):
        for c in range(corners):
            for t in range(tiles):
                at = pl.ds(t * LANES, LANES)
                flat = shift[c, x, :, at] * (per * LANES) + bucket[c, x, :, at]
                if c: flat = pltpu.roll(flat, c * (LANES // corners), axis=1)
                v = (c * nx + x) * tiles + t
                keys[pl.ds(pl.multiple_of(v * SUB, SUB), SUB), :] = flat * (count * SUB) + (sub * count + v)
        return carry
    lax.fori_loop(0, nx, build, 0)
    sort_rows([keys], 32)
    low_bits = int(math.log2(count * SUB * LANES))
    lane = lax.broadcasted_iota(jnp.int32, (SUB, LANES), 1)
    base = jnp.zeros((SUB, LANES), jnp.float32)
    width = jnp.zeros((SUB, 1), jnp.float32)
    for g in range(count // SUB):
        least = (keys[pl.ds(g * SUB * SUB, SUB), :] >> low_bits).astype(jnp.float32)
        most = (keys[pl.ds(g * SUB * SUB + SUB * (SUB - 1), SUB), :] >> low_bits).astype(jnp.float32)
        least = jnp.min(least, axis=1, keepdims=True)
        most = jnp.max(most, axis=1, keepdims=True)
        base = jnp.where(lane == g, least, base)
        width = jnp.maximum(width, most - least + 1.0)
    trips = (width.astype(jnp.int32) + (CHUNK - 1)) // CHUNK
    start = jnp.minimum(base.astype(jnp.int32), rows - trips * CHUNK)
    bounds[...] = jnp.where(lane == LANES - 1, trips, start)


def depart_kernel(heat, picks, rigid, up, down):
    ways = 3
    nx, _, nz = rigid.shape
    tiles = nz // LANES
    narrow = REACH - 2
    per = picks.shape[0] // (ways * ways)
    group = SUB * SUB
    for a, out, first in ((ways - 1, up, nx - narrow), (0, down, 0)):
        start = a * ways * per

        def body(g, carry):
            base = pl.multiple_of(g * group, group)
            found = lookup_all(heat, [picks[pl.ds(start + base + SUB * k, SUB), :] for k in range(SUB)], heat.shape[0])
            for k in range(SUB):
                out[pl.ds(base + SUB * k, SUB), :] = found[k]
            return carry

        lax.fori_loop(0, ways * per // group, body, 0)
        for x in range(narrow):
            for t in range(tiles):
                row = ways * per + (x * tiles + t) * SUB
                out[pl.ds(row, SUB), :] = rigid[first + x, :, pl.ds(t * LANES, LANES)]


def near_kernel(heat, picks, near):
    rows = near.shape[0]
    group = SUB * SUB

    def body(g, carry):
        base = pl.multiple_of(g * group, group)
        found = lookup_all(heat, [picks[pl.ds(rows + base + SUB * k, SUB), :] for k in range(SUB)], heat.shape[0])
        for k in range(SUB):
            near[pl.ds(base + SUB * k, SUB), :] = found[k]
        return carry

    lax.fori_loop(0, rows // group, body, 0)


def forward_kernel(low, near, high, rigid, up, down):
    nx, ny, nz = rigid.shape
    per = near.shape[0] // 3
    narrow = REACH - 2
    tiles = nz // LANES
    extent = nx + 2 * narrow
    for out, b, y in ((up, 2, ny - narrow), (down, 0, 0)):
        for a, ref in enumerate((low, near, high)):
            out[pl.ds(a * per, per), :] = ref[pl.ds(b * per, per), :]
        for t in range(tiles):
            for x in range(extent):
                to = pl.ds(3 * per + (t * extent + x) * narrow, narrow)
                if narrow <= x < narrow + nx:
                    out[to, :] = rigid[x - narrow, pl.ds(y, narrow), pl.ds(t * LANES, LANES)]
                else:
                    ref, k = (low, x) if x < narrow else (high, x - narrow - nx)
                    out[to, :] = ref[pl.ds(3 * per + (k * tiles + t) * SUB + y, narrow), :]


def pick_kernel(left, low, near, high, right, keys, bounds, factor, out, table, position, value):
    corners, nx, _, nz = factor.shape
    tiles = nz // LANES
    slots = near.shape[0] // 3
    for a, ref in enumerate((low, near, high)):
        table[pl.ds((3 * a) * slots, slots), :] = left[pl.ds(a * slots, slots), :]
        table[pl.ds((3 * a + 1) * slots, slots), :] = ref[pl.ds(slots, slots), :]
        table[pl.ds((3 * a + 2) * slots, slots), :] = right[pl.ds(a * slots, slots), :]
    count = keys.shape[0] // SUB
    pos_bits = int(math.log2(count * SUB))
    depth = int(math.log2(CHUNK))
    per = count // SUB

    def body(s, carry):
        own = [keys[pl.ds(SUB * SUB * g + s, SUB, stride=SUB), :] for g in range(per)]
        start = [bounds[s, g] for g in range(per)]

        def step(n, found):
            fresh = []
            for g in range(per):
                lanes = (own[g] >> pos_bits) & (LANES - 1)
                first = start[g] + n * CHUNK
                rel = (own[g] >> (pos_bits + 7)) - first
                bits = [((rel >> b) & 1) == 1 for b in range(depth)]
                fresh.append(jnp.where((rel >> depth) == 0, lookup(table, first, CHUNK, lanes, bits), found[g]))
            return tuple(fresh)

        zero = jnp.zeros((SUB, LANES), jnp.float32)
        found = lax.fori_loop(0, bounds[s, LANES - 1], step, tuple(zero for _ in range(per)))
        for g in range(per):
            at = pl.ds(SUB * SUB * g + s, SUB, stride=SUB)
            value[at, :] = found[g]
            position[at, :] = own[g] & (count * SUB - 1)
        return carry

    lax.fori_loop(0, SUB, body, 0)
    sort_rows([position, value], 16)

    def blend(x, carry):
        for t in range(tiles):
            at = pl.ds(t * LANES, LANES)
            total = None
            for c in range(corners):
                v = (c * nx + x) * tiles + t
                got = value[pl.ds(pl.multiple_of(v * SUB, SUB), SUB), :]
                if c:
                    got = pltpu.roll(got, LANES - c * (LANES // corners), axis=1)
                got = factor[c, x, :, at] * got
                total = got if total is None else total + got
            out[x, :, at] = total
        return carry

    lax.fori_loop(0, nx, blend, 0)


def pack_kernel(width, low, own, high, up, down):
    ny, nz = own.shape[1:]
    extent = low.shape[0] + own.shape[0] + high.shape[0]
    for t in range(nz // LANES):
        at = pl.ds(t * LANES, LANES)
        for x in range(extent):
            ref, k = low, x
            if k >= low.shape[0]:
                ref, k = own, k - low.shape[0]
                if k >= own.shape[0]:
                    ref, k = high, k - own.shape[0]
            to = pl.ds((t * extent + x) * width, width)
            up[to, :] = ref[k, pl.ds(ny - width, width), at]
            down[to, :] = ref[k, pl.ds(0, width), at]


def unpack(target, width, own, dom_low, dom_high, slab_low, slab_high, change):
    nx, ny, nz = own.shape
    tiles = nz // LANES
    extent = nx + 2 * width
    start = REACH - width
    for t in range(tiles):
        for x in range(extent):
            if x < width:
                mine = dom_low(x, t)
            elif x < width + nx:
                mine = own[x - width, :, pl.ds(t * LANES, LANES)]
            else:
                mine = dom_high(x - width - nx, t)
            row = (t * extent + x) * width
            target[t, start + x, pl.ds(SUB, ny), :] = change(mine, start + x, 1)
            target[t, start + x, pl.ds(SUB - width, width), :] = change(slab_low(row), start + x, 0)
            target[t, start + x, pl.ds(SUB + ny, width), :] = change(slab_high(row), start + x, 2)


def krylov_kernel(inside, own, p_low, p_high, p_left, p_right, rigid, d_low, d_high, d_left, d_right,
                  basis, sums, temp, diag, u0, u1, u2, u3):
    nx, ny, nz = own.shape
    tiles = nz // LANES
    parts = temp.shape[2] // SUB
    held = (u0, u1, u2, u3)
    flag = [inside[k].astype(jnp.float32) for k in range(4)]

    def mask(x, part):
        at_x = jnp.where(x < REACH, flag[0], jnp.where(x >= REACH + nx, flag[1], 1.0))
        return at_x * (flag[2] if part == 0 else flag[3] if part == 2 else 1.0)

    temp[...] = jnp.zeros_like(temp)
    wide, narrow = REACH, REACH - 2
    base = d_left.shape[0] - tiles * (nx + 2 * narrow) * narrow

    def plane(ref):
        return lambda x, t: ref[x, :, pl.ds(t * LANES, LANES)]

    def message(ref):
        return lambda x, t: ref[pl.ds(base + (x * tiles + t) * SUB, SUB), :]

    def packed(ref, offset, width):
        return lambda row: ref[pl.ds(offset + row, width), :]

    unpack(temp, wide, own, plane(p_low), plane(p_high), packed(p_left, 0, wide), packed(p_right, 0, wide),
           lambda v, x, part: v)
    diag[...] = jnp.zeros_like(diag)
    unpack(diag, narrow, rigid, message(d_low), message(d_high), packed(d_left, base, narrow),
           packed(d_right, base, narrow),
           lambda v, x, part: (v * (2.0 / HALF) + 2.0 * (6.0 - CENTRE) / HALF) * mask(x, part))
    lane = lax.broadcasted_iota(jnp.int32, (SUB, LANES), 1)
    first, last = lane == 0, lane == LANES - 1
    zero = jnp.zeros((SUB, LANES), jnp.float32)

    def around_z(values):
        back = [pltpu.roll(v, 1, axis=1) for v in values]
        ahead = [pltpu.roll(v, LANES - 1, axis=1) for v in values]
        pairs = []
        for t in range(tiles):
            before = jnp.where(first, back[t - 1] if t else zero, back[t])
            after = jnp.where(last, ahead[t + 1] if t + 1 < tiles else zero, ahead[t])
            pairs.append((before, after))
        return pairs

    def around_y(ref, head, x, part):
        base = part * SUB
        mine = ref[(*head, x, pl.ds(base, SUB))]
        below = pltpu.roll(mine, 1, axis=0) if part == 0 else ref[(*head, x, pl.ds(base - 1, SUB))]
        above = pltpu.roll(mine, SUB - 1, axis=0) if part == parts - 1 else ref[(*head, x, pl.ds(base + 1, SUB))]
        return mine, below, above

    def load_row(x, carry):
        for part in range(parts):
            scale = COEF * mask(x, part)
            rows = [around_y(temp, (t,), x, part) for t in range(tiles)]
            along = around_z([r[0] for r in rows])
            for t in range(tiles):
                ahead = temp[t, x + 1, pl.ds(part * SUB, SUB), :]
                back = temp[t, x - 1, pl.ds(part * SUB, SUB), :]
                u0[0, t, x, pl.ds(part * SUB, SUB), :] = scale * (ahead - back)
                u0[1, t, x, pl.ds(part * SUB, SUB), :] = scale * (rows[t][2] - rows[t][1])
                u0[2, t, x, pl.ds(part * SUB, SUB), :] = scale * (along[t][1] - along[t][0])
        return carry

    lax.fori_loop(1, nx + 2 * REACH - 1, load_row, 0)

    def twice(ref, c, x, part):
        coefficient = (2.0 / HALF) * mask(x, part)
        rows = [around_y(ref, (c, t), x, part) for t in range(tiles)]
        along = around_z([r[0] for r in rows])
        results = []
        for t in range(tiles):
            near = rows[t][1] + rows[t][2] + along[t][0] + along[t][1]
            near = near + ref[c, t, x + 1, pl.ds(part * SUB, SUB), :] + ref[c, t, x - 1, pl.ds(part * SUB, SUB), :]
            results.append(diag[t, x, pl.ds(part * SUB, SUB), :] * rows[t][0] - coefficient * near)
        return results, [r[0] for r in rows]

    for order in range(1, ITERS):
        source, target = held[order - 1], held[order]

        def apply_row(x, carry):
            for c in range(3):
                for part in range(parts):
                    doubled, _ = twice(source, c, x, part)
                    for t in range(tiles):
                        at = (c, t, x, pl.ds(part * SUB, SUB))
                        if order == 1:
                            target[at] = 0.5 * doubled[t]
                        else:
                            target[at] = doubled[t] - held[order - 2][at]
            return carry

        margin = ITERS - order
        lax.fori_loop(REACH - margin, REACH + nx + margin, apply_row, 0)

    def dots_row(x, carry):
        carry = list(carry)
        for c in range(3):
            doubled, u = twice(u3, c, REACH + x, 1)
            for t in range(tiles):
                at = (c, t, REACH + x, pl.ds(SUB, SUB))
                v = [u0[at], u1[at], u2[at], u[t]]
                pairs = [(v[0], v[0]), (v[0], v[1]), (v[1], v[1]), (v[1], v[2]), (v[2], v[2]), (v[2], v[3]),
                         (v[3], v[3]), (v[3], doubled[t])]
                for k, (left, right) in enumerate(pairs):
                    carry[k] = carry[k] + left * right
                for j in range(4):
                    basis[3 * j + c, pl.ds(pl.multiple_of(t * nx * SUB + x * SUB, SUB), SUB), :] = v[j]
        return tuple(carry)

    totals = lax.fori_loop(0, nx, dots_row, tuple(zero for _ in range(8)))
    for k in range(8):
        sums[pl.ds(k, 1), :] = jnp.sum(totals[k], axis=0, keepdims=True)


def surface_kernel(nz, tally, basis, picks, out, index, live):
    fields, rows, _ = basis.shape
    count = picks.shape[0]
    block = rows // (nz // LANES)
    lane = lax.broadcasted_iota(jnp.int32, (1, LANES), 1)
    sub = lax.broadcasted_iota(jnp.int32, (SUB, LANES), 0)
    out[...] = jnp.zeros_like(out)
    for k in range(count):
        spot = picks[k]
        along = spot % nz
        index[pl.ds(k, 1), :] = ((along // LANES) * block + spot // nz) * LANES + spot % LANES
        live[pl.ds(k, 1), :] = (lane < tally[0, k]).astype(jnp.float32)
    depth = int(math.log2(rows))

    def body(f, carry):
        table = basis.at[f]
        spots = index[pl.ds(0, SUB), :]
        high = spots >> 7
        bits = [((high >> bit) & 1) == 1 for bit in range(depth)]
        found = lookup(table, 0, rows, spots & (LANES - 1), bits)
        found = jnp.where(live[pl.ds(0, SUB), :] > 0.5, found, 0.0)
        for k in range(SUB):
            out[pl.ds(SUB + k * fields + f, 1), :] = found[k : k + 1, :]
        for k in range(SUB, count):
            spots = jnp.broadcast_to(index[pl.ds(k, 1), :], (SUB, LANES))
            lanes, high = spots & (LANES - 1), spots >> 7
            total = jnp.zeros((SUB, LANES), jnp.float32)
            for g in range(0, rows, SUB):
                got = jnp.take_along_axis(table[pl.ds(g, SUB), :], lanes, axis=1, mode="promise_in_bounds")
                total = jnp.where(high == sub + g, got, total)
            total = jnp.sum(total, axis=0, keepdims=True)
            total = jnp.where(live[pl.ds(k, 1), :] > 0.5, total, 0.0)
            out[pl.ds(SUB + k * fields + f, 1), :] = total
        return carry

    lax.fori_loop(0, fields, body, 0)


def route_kernel(place, gathered, keep, pair, other):
    peers = gathered.shape[0]
    fields = 3 * ITERS
    total = gathered[0, pl.ds(0, SUB), :]
    for k in range(1, peers):
        total = total + gathered[k, pl.ds(0, SUB), :]
    pair[...] = jnp.zeros_like(pair)
    other[...] = jnp.zeros_like(other)
    pair[pl.ds(0, SUB), :] = total
    odd = place[4]
    for a in range(3):
        source = place[5] + a - 1
        here = jnp.logical_and(source >= 0, source < peers).astype(jnp.float32)
        source = jnp.clip(source, 0, peers - 1)
        rows = [SUB + (3 * (2 - a) + b) * fields for b in range(3)]
        to = pl.ds(SUB + a * fields, fields)
        low = gathered[source, pl.ds(rows[0], fields), :] * here
        high = gathered[source, pl.ds(rows[2], fields), :] * here
        keep[pl.ds(a * fields, fields), :] = gathered[source, pl.ds(rows[1], fields), :] * here
        pair[to, :] = jnp.where(odd == 1, low, high)
        other[to, :] = jnp.where(odd == 1, high, low)


def coefficients(nu):
    half = 0.5

    def gram(i, j):
        return half * (nu[i + j] + nu[abs(i - j)])

    def inner(i, j):
        if j == 0:
            return gram(i, 1)
        return half * (gram(i, j + 1) + gram(i, j - 1))

    def form(vector, matrix):
        n = len(vector)
        total = None
        for i in range(n):
            for j in range(i, n):
                term = vector[i] * vector[j] * matrix(i, j)
                term = term if i == j else 2.0 * term
                total = term if total is None else total + term
        return total

    one = jnp.ones_like(nu[0])
    found, residual, direction = [], [one], [one]
    rr = nu[0]
    for iteration in range(ITERS):
        energy = form(direction, lambda i, j: CENTRE * gram(i, j) + HALF * inner(i, j))
        alpha = rr / energy
        found = [
            (found[i] if i < len(found) else 0.0) + alpha * direction[i] for i in range(len(direction))
        ]
        if iteration + 1 == ITERS:
            break
        image = [CENTRE * d for d in direction] + [jnp.zeros_like(one)]
        for j, d in enumerate(direction):
            if j == 0:
                image[1] = image[1] + HALF * d
            else:
                image[j + 1] = image[j + 1] + half * HALF * d
                image[j - 1] = image[j - 1] + half * HALF * d
        residual = residual + [jnp.zeros_like(one)]
        residual = [r - alpha * w for r, w in zip(residual, image)]
        fresh = form(residual, gram)
        ratio = fresh / rr
        direction = direction + [jnp.zeros_like(one)]
        direction = [r + ratio * d for r, d in zip(residual, direction)]
        rr = fresh
    return found


def finish_kernel(place, keep, pair, sent, other, basis, picks, disp, thermal, shift):
    sums = sent[pl.ds(0, SUB), :] + other[pl.ds(0, SUB), :]
    raw = [jnp.broadcast_to(jnp.sum(sums[k : k + 1, :], axis=1, keepdims=True), (1, LANES)) for k in range(8)]
    nu = [raw[0], raw[1]]
    for k in range(2, 7):
        nu.append(2.0 * raw[k] - raw[k % 2])
    nu.append(2.0 * raw[7] - nu[5] - 2.0 * raw[1])
    weights = coefficients(nu)
    wide = [jnp.broadcast_to(w, (SUB, LANES)) for w in weights]
    _, nx, ny, nz = disp.shape
    tiles = nz // LANES

    def row(x, carry):
        for c in range(3):
            for t in range(tiles):
                at = pl.ds(pl.multiple_of(t * nx * SUB + x * SUB, SUB), SUB)
                total = wide[0] * basis[c, at, :]
                for j in range(1, 4):
                    total = total + wide[j] * basis[3 * j + c, at, :]
                disp[c, x, :, pl.ds(t * LANES, LANES)] = total
        return carry

    lax.fori_loop(0, nx, row, 0)
    depth = thermal.shape[1] // LANES
    fields = 3 * ITERS
    spot_of = lax.broadcasted_iota(jnp.int32, (LANES, LANES), 0)
    tall = lax.broadcasted_iota(jnp.int32, (depth, LANES), 0)
    total = jnp.zeros((9 * depth, LANES), jnp.float32)
    odd = place[4]
    for ref, offset, b, here in (
        (keep, 0, 1, 1),
        (pair, SUB, 2 - 2 * odd, jnp.where(odd == 1, place[2], place[3])),
        (other, SUB, 2 * odd, jnp.where(odd == 1, place[3], place[2])),
    ):
        valid = jnp.full((1, LANES), here, jnp.int32) == 1
        for a in range(3):
            spot = picks[3 * a + b]
            lane_hot = (spot_of == spot % LANES).astype(jnp.float32).astype(jnp.bfloat16)
            row_hot = tall == spot // LANES
            pieces = []
            for c in range(3):
                value = None
                for j in range(ITERS):
                    term = weights[j] * ref[pl.ds(offset + a * fields + 3 * j + c, 1), :]
                    value = term if value is None else value + term
                value = jnp.where(valid, value, 0.0)
                for _ in range(3):
                    part = value.astype(jnp.bfloat16).astype(jnp.float32)
                    value = value - part
                    pieces.append(jnp.where(row_hot, jnp.broadcast_to(part, row_hot.shape), 0.0))
            wanted = jnp.concatenate(pieces, axis=0).astype(jnp.bfloat16)
            total = total + lax.dot_general(wanted, lane_hot, (((1,), (1,)), ((), ())),
                                            preferred_element_type=jnp.float32)
    for c in range(3):
        whole = total[3 * c * depth : (3 * c + 1) * depth]
        whole = whole + total[(3 * c + 1) * depth : (3 * c + 2) * depth]
        shift[...] = whole + total[(3 * c + 2) * depth : (3 * c + 3) * depth]
        for r in range(depth):
            thermal[pl.ds(c, 1), pl.ds(r * LANES, LANES)] = shift[pl.ds(r, 1), :]


def swap(last, leading, axis):
    peers = lax.axis_size(axis)
    up = [(i, i + 1) for i in range(peers - 1)]
    down = [(j, i) for i, j in up]
    return lax.ppermute(last, axis, up), lax.ppermute(leading, axis, down)


def on_device(heat_level, emitting, holder, bucket, factors, rigidity, boundary, tally, accepting):
    f32, i32 = jnp.float32, jnp.int32
    ways = emitting.shape[1]
    per = emitting.shape[3] // LANES
    nx, ny, nz = rigidity.shape
    tiles = nz // LANES
    narrow = REACH - 2
    call = pl.pallas_call
    shape = jax.ShapeDtypeStruct
    dom, slab = lax.axis_index("dom"), lax.axis_index("slab")
    place = jnp.stack([dom > 0, dom < lax.axis_size("dom") - 1, slab > 0, slab < lax.axis_size("slab") - 1,
                       slab % 2, dom]).astype(i32)
    heat = heat_level.reshape(-1, LANES)
    emit_rows = emitting.reshape(-1, LANES)
    dom_message = shape((ways * per + narrow * tiles * ny, LANES), f32)
    up, down = call(depart_kernel, out_shape=(dom_message,) * 2, in_specs=[VMEM] * 3, out_specs=(VMEM,) * 2,
                    compiler_params=params(6), cost_estimate=cost(8), name="depart")(heat, emit_rows, rigidity)
    from_low, from_high = swap(up, down, "dom")
    near = call(near_kernel, out_shape=shape((ways * per, LANES), f32), in_specs=[VMEM] * 2, out_specs=VMEM,
                compiler_params=params(4), cost_estimate=cost(4), name="near")(heat, emit_rows)
    count = holder.size // LANES
    rows = ways * ways * per
    keys, bounds = call(
        functools.partial(plan_kernel, per, rows),
        out_shape=(shape((count, LANES), i32), shape((SUB, LANES), i32)),
        in_specs=[VMEM] * 2, out_specs=(VMEM, VMEM), compiler_params=params(6), cost_estimate=cost(5), name="plan",
    )(holder, bucket)
    slab_message = shape((ways * per + tiles * (nx + 2 * narrow) * narrow, LANES), f32)
    up, down = call(forward_kernel, out_shape=(slab_message,) * 2, in_specs=[VMEM] * 4, out_specs=(VMEM,) * 2,
                    compiler_params=params(6), cost_estimate=cost(1), name="forward")(from_low, near, from_high, rigidity)
    left, right = swap(up, down, "slab")
    interp = call(
        pick_kernel, out_shape=shape((nx, ny, nz), f32), in_specs=[VMEM] * 6 + [SMEM, VMEM], out_specs=VMEM,
        scratch_shapes=[pltpu.VMEM((rows, LANES), f32), pltpu.VMEM((count, LANES), i32), pltpu.VMEM((count, LANES), f32)],
        compiler_params=params(8), cost_estimate=cost(14), name="pick",
    )(left, from_low, near, from_high, right, keys, bounds, factors)
    p_low, p_high = swap(interp[nx - REACH :], interp[:REACH], "dom")
    halo = shape((tiles * (nx + 2 * REACH) * REACH, LANES), f32)
    up, down = call(functools.partial(pack_kernel, REACH), out_shape=(halo, halo), in_specs=[VMEM] * 3,
                    out_specs=(VMEM, VMEM), compiler_params=params(6), cost_estimate=cost(1), name="pack")(p_low, interp, p_high)
    p_left, p_right = swap(up, down, "slab")
    extent = nx + 2 * REACH
    field = pltpu.VMEM((3, tiles, extent, 3 * SUB, LANES), f32)
    basis, sums = call(
        krylov_kernel,
        out_shape=(shape((3 * ITERS, tiles * nx * ny, LANES), f32), shape((SUB, LANES), f32)),
        in_specs=[SMEM] + [VMEM] * 10,
        out_specs=(VMEM, VMEM),
        scratch_shapes=[pltpu.VMEM((tiles, extent, 3 * SUB, LANES), f32)] * 2 + [field] * 4,
        compiler_params=params(20), cost_estimate=cost(7), name="krylov",
    )(place, interp, p_low, p_high, p_left, p_right, rigidity, from_low, from_high, left, right)
    peers = lax.axis_size("slab")
    hop = peers // 2
    while hop >= 4:
        sums = sums + lax.ppermute(sums, "slab", [(i, (i + hop) % peers) for i in range(peers)])
        hop //= 2
    fields = 3 * ITERS
    length = SUB + -(-ways * ways * fields // SUB) * SUB
    surface = call(
        functools.partial(surface_kernel, nz), out_shape=shape((length, LANES), f32), in_specs=[SMEM, VMEM, VMEM],
        out_specs=VMEM, scratch_shapes=[pltpu.VMEM((2 * SUB, LANES), i32), pltpu.VMEM((2 * SUB, LANES), f32)],
        compiler_params=params(6), cost_estimate=cost(4), name="surface",
    )(tally, basis, boundary.reshape(-1, 1, LANES))
    gathered = lax.all_gather(lax.dynamic_update_slice(surface, sums, (0, 0)), "dom")
    short = -(-ways * fields // SUB) * SUB
    message = shape((SUB + short, LANES), f32)
    keep, pair, other = call(
        route_kernel, out_shape=(shape((short, LANES), f32), message, message), in_specs=[SMEM, VMEM],
        out_specs=(VMEM,) * 3, compiler_params=params(4), cost_estimate=cost(1), name="route",
    )(place, gathered)
    pair_in = lax.ppermute(pair, "slab", [(i, i ^ 1) for i in range(peers)])
    sent = lax.dynamic_update_slice(other, pair[:SUB] + pair_in[:SUB], (0, 0))
    rounds = [(i, (i + 1) % peers if i % 2 else (i - 1) % peers) for i in range(peers)]
    other_in = lax.ppermute(sent, "slab", rounds)
    return call(
        finish_kernel,
        out_shape=(shape((3, nx, ny, nz), f32), shape((3, heat_level.shape[0]), f32)),
        in_specs=[SMEM] + [VMEM] * 6,
        out_specs=(VMEM, VMEM),
        scratch_shapes=[pltpu.VMEM((heat_level.shape[0] // LANES, LANES), f32)],
        compiler_params=params(8), cost_estimate=cost(2), name="finish",
    )(place, keep, pair_in, sent, other_in, basis, accepting.reshape(-1, 1, LANES))


def solution(mesh):
    both = ("dom", "slab")
    in_specs = (
        P(both),
        P(both, None, None, None),
        P(None, "dom", "slab", None),
        P(None, "dom", "slab", None),
        P(None, "dom", "slab", None),
        P("dom", "slab", None),
        P(both, None, None, None),
        P(both, None),
        P(both, None, None, None),
    )
    out_specs = (P(None, "dom", "slab", None), P(None, both))
    return jax.shard_map(on_device, mesh=mesh, in_specs=in_specs, out_specs=out_specs, check_vma=False)
```

```python
import functools
import math

import jax
import jax.numpy as jnp
from jax import lax
from jax.experimental import pallas as pl
from jax.experimental.pallas import tpu as pltpu
from jax.sharding import PartitionSpec as P

ITERS = 4
COEF = 0.5
LANES = 128
CHUNK = 16
WEIGHT = 4e8
DEPART_MIB = 56
SUB = 8
CENTRE = 7.125
HALF = 6.875
REACH = ITERS + 1
VMEM = pl.BlockSpec(memory_space=pltpu.VMEM)
SMEM = pl.BlockSpec(memory_space=pltpu.SMEM)
HBM = pl.BlockSpec(memory_space=pltpu.HBM)


def params(mib):
    return pltpu.CompilerParams(vmem_limit_bytes=mib * 1024 * 1024)


def cost(micro, moved=0):
    return pl.CostEstimate(flops=int(micro * WEIGHT), bytes_accessed=moved, transcendentals=0)


def permute(value, lanes):
    return jnp.take_along_axis(value, lanes, axis=1, mode="promise_in_bounds")


def mix(values):
    tiles = len(values)
    lane = lax.broadcasted_iota(jnp.int32, values[0].shape, 1)
    share = LANES // tiles
    mixed = []
    for t in range(tiles):
        source = (lane * tiles + t) % LANES
        total = permute(values[0], source)
        for k in range(1, tiles):
            total = jnp.where(lane >= k * share, permute(values[k], source), total)
        mixed.append(total)
    return mixed


def unmix(values):
    tiles = len(values)
    lane = lax.broadcasted_iota(jnp.int32, values[0].shape, 1)
    share = LANES // tiles
    plain = []
    for k in range(tiles):
        source = k * share + lane // tiles
        total = permute(values[0], source)
        for t in range(1, tiles):
            total = jnp.where(lane % tiles == t, permute(values[t], source), total)
        plain.append(total)
    return plain


def wedge(nx, reach):
    rows, offset = [], 0
    for x in range(1 - reach, nx + reach - 1):
        width = reach - max(0, -x, x - nx + 1)
        rows.append((x, width, offset))
        offset += width
    return rows, offset


def lookup(table, first, rows, lanes, bits):
    if rows == 1:
        row = jnp.broadcast_to(table[pl.ds(first, 1), :], lanes.shape)
        return jnp.take_along_axis(row, lanes, axis=1, mode="promise_in_bounds")
    half = rows // 2
    lower = lookup(table, first, half, lanes, bits[:-1])
    upper = lookup(table, first + half, half, lanes, bits[:-1])
    return jnp.where(bits[-1], upper, lower)


def lookup_all(table, indices, chunk):
    rows = table.shape[0]
    depth = int(math.log2(chunk))
    lanes = [index & (LANES - 1) for index in indices]
    high = [index >> 7 for index in indices]
    outer = [value >> depth for value in high]

    def step(block, found):
        base = pl.multiple_of(block * chunk, chunk)
        fresh = []
        for lane, value, top, old in zip(lanes, high, outer, found):
            bits = [((value >> bit) & 1) == 1 for bit in range(depth)]
            fresh.append(jnp.where(top == block, lookup(table, base, chunk, lane, bits), old))
        return tuple(fresh)

    zero = jnp.zeros(indices[0].shape, jnp.float32)
    return lax.fori_loop(0, rows // chunk, step, tuple(zero for _ in indices))


def order2(a, b):
    if len(a) == 1:
        return (jnp.minimum(a[0], b[0]),), (jnp.maximum(a[0], b[0]),)
    swap = a[0] > b[0]
    low = [jnp.minimum(a[0], b[0])] + [jnp.where(swap, y, x) for x, y in zip(a[1:], b[1:])]
    high = [jnp.maximum(a[0], b[0])] + [jnp.where(swap, x, y) for x, y in zip(a[1:], b[1:])]
    return tuple(low), tuple(high)


def sublane_xor(value, mask):
    sub = lax.broadcasted_iota(jnp.int32, value.shape, 0)
    return jnp.take_along_axis(value, sub ^ mask, axis=0, mode="promise_in_bounds")


def keep_one(a, other, lower):
    if len(a) == 1:
        return (jnp.where(lower, jnp.minimum(a[0], other[0]), jnp.maximum(a[0], other[0])),)
    take = (a[0] > other[0]) == lower
    return tuple(jnp.where(take, y, x) for x, y in zip(a, other))


def sort_rows(refs, block, done=0, until=None):
    count = refs[0].shape[0] // SUB

    def load(v):
        at = pl.ds(pl.multiple_of(v * SUB, SUB), SUB)
        return tuple(r[at, :] for r in refs)

    def store(v, value):
        at = pl.ds(pl.multiple_of(v * SUB, SUB), SUB)
        for r, x in zip(refs, value): r[at, :] = x

    def strides(held, stride):
        while stride:
            for i in range(len(held)):
                if not i & stride:
                    held[i], held[i | stride] = order2(held[i], held[i | stride])
            stride //= 2

    def whole(t, carry):
        held = [load(t * block + i) for i in range(block)]
        size = 2
        while size <= block:
            for i in range(block):
                j = i ^ (size - 1)
                if i < j: held[i], held[j] = order2(held[i], held[j])
            strides(held, size // 4)
            size *= 2
        for i in range(block): store(t * block + i, held[i])
        return carry

    def finish(t, carry):
        held = [load(t * block + i) for i in range(block)]
        strides(held, block // 2)
        for i in range(block): store(t * block + i, held[i])
        return carry

    if not done:
        lax.fori_loop(0, count // block, whole, 0)
    size = 2 * max(done, block)
    while size <= (until or count * SUB):
        span = min(size, count)
        flip = size // count - 1 if size > count else 0
        groups = span // block

        def top(t, carry):
            base = (t // (block // 2)) * span
            i = t % (block // 2)
            spots = []
            for j in range(groups):
                spots += [base + i + block * j, base + block - 1 - i + block * j]
            held = [load(v) for v in spots]
            n = len(held)
            if flip:
                sub = lax.broadcasted_iota(jnp.int32, (SUB, LANES), 0)
                lower = (sub & ((flip + 1) // 2)) == 0
                turned = [tuple(sublane_xor(x, flip) for x in h) for h in held]
                held = [keep_one(held[k], turned[n - 1 - k], lower) for k in range(n)]
                bit = (flip + 1) // 4
                while bit:
                    lower = (sub & bit) == 0
                    held = [keep_one(h, tuple(sublane_xor(x, bit) for x in h), lower) for h in held]
                    bit //= 2
                far = groups // 2
            else:
                for k in range(n // 2):
                    held[k], held[n - 1 - k] = order2(held[k], held[n - 1 - k])
                far = groups // 4
            while far:
                for j in range(groups):
                    if not j & far:
                        for side in range(2):
                            x, y = 2 * j + side, 2 * (j | far) + side
                            held[x], held[y] = order2(held[x], held[y])
                far //= 2
            for v, h in zip(spots, held): store(v, h)
            return carry

        lax.fori_loop(0, (count // span) * (block // 2), top, 0, unroll=max(1, 8 // groups))
        lax.fori_loop(0, count // block, finish, 0)
        size *= 2


def blocks_of(place):
    kinds = 1 + place[0] + place[1]
    return kinds, 1 - place[0], 2 - place[4], 1 + place[4]


def plan_kernel(per, place, shift, bucket, keys):
    kinds, first, left, right = blocks_of(place)
    corners, nx, _, nz = shift.shape
    tiles = nz // LANES
    count = corners * nx * tiles
    sub = lax.broadcasted_iota(jnp.int32, (SUB, LANES), 0)

    def build(x, carry):
        for c in range(corners):
            for t in range(tiles):
                at = pl.ds(t * LANES, LANES)
                way = shift[c, x, :, at]
                a = (way * 11) >> 5
                b = way - 3 * a
                block = jnp.where(b == 1, 0, jnp.where(b == 0, left * kinds, right * kinds)) + (a - first)
                flat = block * (per * LANES) + bucket[c, x, :, at]
                if c:
                    flat = pltpu.roll(flat, c * (LANES // corners), axis=1)
                v = (c * nx + x) * tiles + t
                keys[pl.ds(pl.multiple_of(v * SUB, SUB), SUB), :] = flat * (count * SUB) + (sub * count + v)
        return carry

    lax.fori_loop(0, nx, build, 0)
    sort_rows([keys], 32, until=count)


def order_kernel(per, place, begun, keys, bounds):
    keys[...] = begun[...]
    count = keys.shape[0] // SUB
    sort_rows([keys], 32, done=count)
    low_bits = int(math.log2(count * SUB * LANES))
    lane = lax.broadcasted_iota(jnp.int32, (SUB, LANES), 1)
    base = jnp.zeros((SUB, LANES), jnp.float32)
    width = jnp.zeros((SUB, 1), jnp.float32)
    top = jnp.zeros((SUB, 1), jnp.float32)
    for g in range(count // SUB):
        least = (keys[pl.ds(g * SUB * SUB, SUB), :] >> low_bits).astype(jnp.float32)
        most = (keys[pl.ds(g * SUB * SUB + SUB * (SUB - 1), SUB), :] >> low_bits).astype(jnp.float32)
        least = jnp.min(least, axis=1, keepdims=True)
        most = jnp.max(most, axis=1, keepdims=True)
        base = jnp.where(lane == g, least, base)
        width = jnp.maximum(width, most - least + 1.0)
        top = jnp.maximum(top, most)
    trips = (width.astype(jnp.int32) + (CHUNK - 1)) // CHUNK
    ready = 2 * blocks_of(place)[0] * per
    rows = jnp.where(top.astype(jnp.int32) < ready, ready, 9 * per)
    start = jnp.minimum(base.astype(jnp.int32), rows - trips * CHUNK)
    latest = jnp.max(jnp.where(lane < count // SUB, start, 0).astype(jnp.float32), axis=1, keepdims=True)
    soon = jnp.clip((ready - latest.astype(jnp.int32)) // CHUNK, 0, trips)
    bounds[...] = jnp.where(lane == LANES - 1, trips, jnp.where(lane == LANES - 2, soon, start))


def visit(table, keys, bounds, soon, before, store):
    count = keys.shape[0] // SUB
    pos_bits = int(math.log2(count * SUB))
    depth = int(math.log2(CHUNK))
    per = count // SUB

    def body(s, carry):
        own = [keys[pl.ds(SUB * SUB * g + s, SUB, stride=SUB), :] for g in range(per)]
        start = [bounds[s, g] for g in range(per)]

        def step(n, found):
            fresh = []
            for g in range(per):
                lanes = (own[g] >> pos_bits) & (LANES - 1)
                first = start[g] + n * CHUNK
                rel = (own[g] >> (pos_bits + 7)) - first
                bits = [((rel >> b) & 1) == 1 for b in range(depth)]
                fresh.append(jnp.where((rel >> depth) == 0, lookup(table, first, CHUNK, lanes, bits), found[g]))
            return tuple(fresh)

        spots = [pl.ds(SUB * SUB * g + s, SUB, stride=SUB) for g in range(per)]
        least = 0 if soon else bounds[s, LANES - 2]
        most = bounds[s, LANES - 2 if soon else LANES - 1]
        found = lax.fori_loop(least, most, step, tuple(before(at) for at in spots))
        for g, at in enumerate(spots):
            store(at, found[g], own[g] & (count * SUB - 1))
        return carry

    lax.fori_loop(0, SUB, body, 0)


def slots_of(heat, picks, first, out, rows):
    group = SUB * SUB

    def body(g, carry):
        base = pl.multiple_of(g * group, group)
        found = lookup_all(heat, [picks[pl.ds(first + base + SUB * k, SUB), :] for k in range(SUB)], heat.shape[0])
        for k in range(SUB):
            out[pl.ds(base + SUB * k, SUB), :] = found[k]
        return carry

    lax.fori_loop(0, rows // group, body, 0)


def depart_kernel(heat_hbm, picks_hbm, rigid_hbm, up, mixed, heat, picks, rigid, arrived):
    rows = picks.shape[0]
    sources = (rigid_hbm, heat_hbm, picks_hbm.at[pl.ds(picks_hbm.shape[0] - rows, rows), :])
    copies = [
        pltpu.make_async_copy(source, target, arrived.at[k])
        for k, (source, target) in enumerate(zip(sources, (rigid, heat, picks)))
    ]
    for copy in copies:
        copy.start()
    nx, _, nz = rigid.shape
    tiles = nz // LANES
    narrow = REACH - 2
    copies[0].wait()
    for x in range(nx):
        values = mix([rigid[x, :, pl.ds(t * LANES, LANES)] for t in range(tiles)])
        for t in range(tiles):
            mixed[x, pl.ds(t * SUB, SUB), :] = values[t]
            if x >= nx - narrow:
                up[pl.ds(rows + ((x - nx + narrow) * tiles + t) * SUB, SUB), :] = values[t]
    copies[1].wait()
    copies[2].wait()
    slots_of(heat, picks, 0, up, rows)


def depart_down_kernel(heat, picks, mixed, down):
    narrow = REACH - 2
    tall = mixed.shape[1]
    rows = down.shape[0] - narrow * tall
    for x in range(narrow):
        down[pl.ds(rows + x * tall, tall), :] = mixed[x]
    slots_of(heat, picks, 0, down, rows)


def near_kernel(heat, picks, near):
    slots_of(heat, picks, near.shape[0], near, near.shape[0])


def forward_kernel(place, low, near, high, rigid, pair, other):
    nx, ny = rigid.shape[0], SUB
    per = near.shape[0] // 3
    tiles = rigid.shape[1] // SUB
    odd = place[4] == 1
    rows, size = wedge(nx, REACH - 2)

    def give(to, up, down):
        pair[to, :] = jnp.where(odd, down, up)
        other[to, :] = jnp.where(odd, up, down)

    for a, ref in enumerate((low, near, high)):
        give(pl.ds(a * per, per), ref[pl.ds(2 * per, per), :], ref[pl.ds(0, per), :])
    for t in range(tiles):
        for x, width, offset in rows:
            to = pl.ds(3 * per + t * size + offset, width)
            if 0 <= x < nx:
                base = t * SUB
                give(to, rigid[x, pl.ds(base + ny - width, width), :], rigid[x, pl.ds(base, width), :])
            else:
                ref, k = (low, x + REACH - 2) if x < 0 else (high, x - nx)
                base = 3 * per + (k * tiles + t) * SUB
                give(to, ref[pl.ds(base + ny - width, width), :], ref[pl.ds(base, width), :])


def lay(table, per, place, columns):
    kinds, first = blocks_of(place)[:2]
    for valid, column, readers in columns:
        for a, read in enumerate(readers):
            here = valid if a == 1 else jnp.logical_and(valid, place[0 if a == 0 else 1] == 1)

            @pl.when(here)
            def _():
                row = pl.multiple_of((column * kinds + a - first) * per, per)
                table[pl.ds(row, per), :] = read()


def early_kernel(place, pair, low, near, high, keys, bounds, value, table):
    per = near.shape[0] // 3
    own = [lambda ref=ref: ref[pl.ds(per, per), :] for ref in (low, near, high)]
    side = [lambda at=pl.ds(a * per, per): pair[at, :] for a in range(3)]
    lay(table, per, place, [(place[0] >= 0, 0, own), (place[0] >= 0, 1, side)])

    def store(at, found, spot):
        value[at, :] = found

    visit(table, keys, bounds, True, lambda at: jnp.zeros((SUB, LANES), jnp.float32), store)


def pick_kernel(place, pair, other, low, near, high, keys, early, bounds, factor, out, table, position, value):
    odd = place[4] == 1
    corners, nx, _, nz = factor.shape
    tiles = nz // LANES
    slots = near.shape[0] // 3
    own = [lambda ref=ref: ref[pl.ds(slots, slots), :] for ref in (low, near, high)]

    def side(even_ref, odd_ref):
        return [lambda at=pl.ds(a * slots, slots): jnp.where(odd, odd_ref[at, :], even_ref[at, :]) for a in range(3)]

    _, _, left, right = blocks_of(place)
    lay(table, slots, place, [(place[0] >= 0, 0, own), (place[2] == 1, left, side(other, pair)),
                              (place[3] == 1, right, side(pair, other))])

    def store(at, found, spot):
        value[at, :] = found
        position[at, :] = spot

    visit(table, keys, bounds, False, lambda at: early[at, :], store)
    sort_rows([position, value], 16)

    def blend(x, carry):
        blended = []
        for t in range(tiles):
            at = pl.ds(t * LANES, LANES)
            total = None
            for c in range(corners):
                v = (c * nx + x) * tiles + t
                got = value[pl.ds(pl.multiple_of(v * SUB, SUB), SUB), :]
                if c:
                    got = pltpu.roll(got, LANES - c * (LANES // corners), axis=1)
                got = factor[c, x, :, at] * got
                total = got if total is None else total + got
            blended.append(total)
        for t, total in enumerate(mix(blended)):
            out[x, pl.ds(t * SUB, SUB), :] = total
        return carry

    lax.fori_loop(0, nx, blend, 0)


def pack_kernel(place, low, own, high, pair, other):
    nx, ny = own.shape[0], SUB
    tiles = own.shape[1] // SUB
    odd = place[4] == 1
    rows, size = wedge(nx, REACH)
    for t in range(tiles):
        for x, width, offset in rows:
            ref, k = (own, x) if 0 <= x < nx else (low, x + REACH) if x < 0 else (high, x - nx)
            up = ref[k, pl.ds(t * SUB + ny - width, width), :]
            down = ref[k, pl.ds(t * SUB, width), :]
            to = pl.ds(t * size + offset, width)
            pair[to, :] = jnp.where(odd, down, up)
            other[to, :] = jnp.where(odd, up, down)


def unpack(target, reach, own, dom_low, dom_high, pair, other, offset, odd, change):
    nx = own.shape[0]
    tiles = own.shape[1] // SUB
    rows, size = wedge(nx, reach)
    for t in range(tiles):
        for x in range(-reach, nx + reach):
            if 0 <= x < nx:
                mine = own[x, pl.ds(t * SUB, SUB), :]
            else:
                mine = dom_low(x + reach, t) if x < 0 else dom_high(x - nx, t)
            target[t, REACH + x, pl.ds(SUB, SUB), :] = change(mine, REACH + x, 1)
        for x, width, row in rows:
            at = pl.ds(offset + t * size + row, width)
            even_low, odd_low = other[at, :], pair[at, :]
            target[t, REACH + x, pl.ds(SUB - width, width), :] = change(jnp.where(odd, odd_low, even_low), REACH + x, 0)
            target[t, REACH + x, pl.ds(2 * SUB, width), :] = change(jnp.where(odd, even_low, odd_low), REACH + x, 2)


def krylov_kernel(inside, own, p_low, p_high, p_pair, p_other, rigid, d_low, d_high, d_pair, d_other,
                  basis, sums, temp, diag, u0, u1, u2, u3):
    nx = own.shape[0]
    tiles = own.shape[1] // SUB
    parts = temp.shape[2] // SUB
    held = (u0, u1, u2, u3)
    flag = [inside[k].astype(jnp.float32) for k in range(4)]

    def mask(x, part):
        at_x = jnp.where(x < REACH, flag[0], jnp.where(x >= REACH + nx, flag[1], 1.0))
        return at_x * (flag[2] if part == 0 else flag[3] if part == 2 else 1.0)

    temp[...] = jnp.zeros_like(temp)
    odd = inside[4] == 1
    base = d_pair.shape[0] - tiles * wedge(nx, REACH - 2)[1]
    first_d = d_low.shape[0] - tiles * SUB * (REACH - 2)

    def plane(ref):
        return lambda x, t: ref[x, pl.ds(t * SUB, SUB), :]

    def message(ref):
        return lambda x, t: ref[pl.ds(first_d + (x * tiles + t) * SUB, SUB), :]

    unpack(temp, REACH, own, plane(p_low), plane(p_high), p_pair, p_other, 0, odd, lambda v, x, part: v)
    diag[...] = jnp.zeros_like(diag)
    unpack(diag, REACH - 2, rigid, message(d_low), message(d_high), d_pair, d_other, base, odd,
           lambda v, x, part: (v * (2.0 / HALF) + 2.0 * (6.0 - CENTRE) / HALF) * mask(x, part))
    lane = lax.broadcasted_iota(jnp.int32, (SUB, LANES), 1)
    first, last = lane == 0, lane == LANES - 1
    zero = jnp.zeros((SUB, LANES), jnp.float32)

    def around_z(values):
        back = jnp.where(first, zero, pltpu.roll(values[-1], 1, axis=1))
        ahead = jnp.where(last, zero, pltpu.roll(values[0], LANES - 1, axis=1))
        return [(values[t - 1] if t else back, values[t + 1] if t + 1 < tiles else ahead) for t in range(tiles)]

    def around_y(ref, head, x, part):
        base = part * SUB
        mine = ref[(*head, x, pl.ds(base, SUB))]
        below = pltpu.roll(mine, 1, axis=0) if part == 0 else ref[(*head, x, pl.ds(base - 1, SUB))]
        above = pltpu.roll(mine, SUB - 1, axis=0) if part == parts - 1 else ref[(*head, x, pl.ds(base + 1, SUB))]
        return mine, below, above

    def load_row(x, carry):
        for part in range(parts):
            scale = COEF * mask(x, part)
            rows = [around_y(temp, (t,), x, part) for t in range(tiles)]
            along = around_z([r[0] for r in rows])
            for t in range(tiles):
                ahead = temp[t, x + 1, pl.ds(part * SUB, SUB), :]
                back = temp[t, x - 1, pl.ds(part * SUB, SUB), :]
                u0[0, t, x, pl.ds(part * SUB, SUB), :] = scale * (ahead - back)
                u0[1, t, x, pl.ds(part * SUB, SUB), :] = scale * (rows[t][2] - rows[t][1])
                u0[2, t, x, pl.ds(part * SUB, SUB), :] = scale * (along[t][1] - along[t][0])
        return carry

    lax.fori_loop(1, nx + 2 * REACH - 1, load_row, 0)

    def twice(ref, c, x, part):
        coefficient = (2.0 / HALF) * mask(x, part)
        rows = [around_y(ref, (c, t), x, part) for t in range(tiles)]
        along = around_z([r[0] for r in rows])
        results = []
        for t in range(tiles):
            near = rows[t][1] + rows[t][2] + along[t][0] + along[t][1]
            near = near + ref[c, t, x + 1, pl.ds(part * SUB, SUB), :] + ref[c, t, x - 1, pl.ds(part * SUB, SUB), :]
            results.append(diag[t, x, pl.ds(part * SUB, SUB), :] * rows[t][0] - coefficient * near)
        return results, [r[0] for r in rows]

    for order in range(1, ITERS):
        source, target = held[order - 1], held[order]

        def apply_row(x, carry):
            for c in range(3):
                for part in range(parts):
                    doubled, _ = twice(source, c, x, part)
                    for t in range(tiles):
                        at = (c, t, x, pl.ds(part * SUB, SUB))
                        if order == 1:
                            target[at] = 0.5 * doubled[t]
                        else:
                            target[at] = doubled[t] - held[order - 2][at]
            return carry

        margin = ITERS - order
        lax.fori_loop(REACH - margin, REACH + nx + margin, apply_row, 0)

    def dots_row(x, carry):
        carry = list(carry)
        for c in range(3):
            doubled, u = twice(u3, c, REACH + x, 1)
            for t in range(tiles):
                at = (c, t, REACH + x, pl.ds(SUB, SUB))
                v = [u0[at], u1[at], u2[at], u[t]]
                pairs = [(v[0], v[0]), (v[0], v[1]), (v[1], v[1]), (v[1], v[2]), (v[2], v[2]), (v[2], v[3]),
                         (v[3], v[3]), (v[3], doubled[t])]
                for k, (left, right) in enumerate(pairs):
                    carry[k] = carry[k] + left * right
                for j in range(4):
                    basis[3 * j + c, pl.ds(pl.multiple_of(t * nx * SUB + x * SUB, SUB), SUB), :] = v[j]
        return tuple(carry)

    totals = lax.fori_loop(0, nx, dots_row, tuple(zero for _ in range(8)))
    for k in range(8):
        sums[pl.ds(k, 1), :] = jnp.sum(totals[k], axis=0, keepdims=True)


def surface_kernel(nz, tally, place, basis, picks, keep, pair, other, index, live):
    fields, rows, _ = basis.shape
    count = picks.shape[0]
    tiles = nz // LANES
    block = rows // tiles
    odd = place[6] == 1
    lane = lax.broadcasted_iota(jnp.int32, (1, LANES), 1)
    sub = lax.broadcasted_iota(jnp.int32, (SUB, LANES), 0)
    for k in range(count):
        spot = picks[k]
        along = spot % nz
        index[pl.ds(k, 1), :] = ((along % tiles) * block + spot // nz) * LANES + along // tiles
        live[pl.ds(k, 1), :] = (lane < tally[0, k]).astype(jnp.float32)

    def give(f, values):
        for b in range(3):
            keep[pl.ds(b * fields + f, 1), :] = values[3 + b]
            to = pl.ds(SUB + b * fields + f, 1)
            pair[to, :] = jnp.where(odd, values[b], values[6 + b])
            other[to, :] = jnp.where(odd, values[6 + b], values[b])

    depth = int(math.log2(rows))

    def body(f, carry):
        table = basis.at[f]
        spots = index[pl.ds(0, SUB), :]
        high = spots >> 7
        bits = [((high >> bit) & 1) == 1 for bit in range(depth)]
        found = lookup(table, 0, rows, spots & (LANES - 1), bits)
        found = jnp.where(live[pl.ds(0, SUB), :] > 0.5, found, 0.0)
        values = [found[k : k + 1, :] for k in range(SUB)]
        for k in range(SUB, count):
            spots = jnp.broadcast_to(index[pl.ds(k, 1), :], (SUB, LANES))
            lanes, high = spots & (LANES - 1), spots >> 7
            total = jnp.zeros((SUB, LANES), jnp.float32)
            for g in range(0, rows, SUB):
                got = jnp.take_along_axis(table[pl.ds(g, SUB), :], lanes, axis=1, mode="promise_in_bounds")
                total = jnp.where(high == sub + g, got, total)
            total = jnp.sum(total, axis=0, keepdims=True)
            total = jnp.where(live[pl.ds(k, 1), :] > 0.5, total, 0.0)
            values.append(total)
        give(f, values)
        return carry

    lax.fori_loop(0, fields, body, 0)


def route_kernel(place, kept, pair_in, sent, other_in, keep, pair, other):
    fields = 3 * ITERS
    pair[pl.ds(0, SUB), :] = sent[pl.ds(0, SUB), :] + other_in[pl.ds(0, SUB), :]
    odd, odd_dom = place[4] == 1, place[6] == 1
    for b in range(3):
        at = pl.ds(SUB + b * fields, fields)
        one, two = pair_in[at, :], other_in[at, :]
        low = jnp.where(odd_dom, one, two) * place[0].astype(jnp.float32)
        high = jnp.where(odd_dom, two, one) * place[1].astype(jnp.float32)
        for a, rows in ((0, low), (1, kept[pl.ds(b * fields, fields), :]), (2, high)):
            if b == 1:
                keep[pl.ds(a * fields, fields), :] = rows
            else:
                to = pl.ds(SUB + a * fields, fields)
                chosen = odd if b == 0 else jnp.logical_not(odd)

                @pl.when(chosen)
                def _():
                    pair[to, :] = rows

                @pl.when(jnp.logical_not(chosen))
                def _():
                    other[to, :] = rows


def coefficients(nu):
    half = 0.5

    def gram(i, j):
        return half * (nu[i + j] + nu[abs(i - j)])

    def inner(i, j):
        if j == 0:
            return gram(i, 1)
        return half * (gram(i, j + 1) + gram(i, j - 1))

    def form(vector, matrix):
        n = len(vector)
        total = None
        for i in range(n):
            for j in range(i, n):
                term = vector[i] * vector[j] * matrix(i, j)
                term = term if i == j else 2.0 * term
                total = term if total is None else total + term
        return total

    one = jnp.ones_like(nu[0])
    found, residual, direction = [], [one], [one]
    rr = nu[0]
    for iteration in range(ITERS):
        energy = form(direction, lambda i, j: CENTRE * gram(i, j) + HALF * inner(i, j))
        alpha = rr / energy
        found = [
            (found[i] if i < len(found) else 0.0) + alpha * direction[i] for i in range(len(direction))
        ]
        if iteration + 1 == ITERS:
            break
        image = [CENTRE * d for d in direction] + [jnp.zeros_like(one)]
        for j, d in enumerate(direction):
            if j == 0:
                image[1] = image[1] + HALF * d
            else:
                image[j + 1] = image[j + 1] + half * HALF * d
                image[j - 1] = image[j - 1] + half * HALF * d
        residual = residual + [jnp.zeros_like(one)]
        residual = [r - alpha * w for r, w in zip(residual, image)]
        fresh = form(residual, gram)
        ratio = fresh / rr
        direction = direction + [jnp.zeros_like(one)]
        direction = [r + ratio * d for r, d in zip(residual, direction)]
        rr = fresh
    return found


def hot_kernel(picks, row_hot, lane_hot):
    count = picks.shape[0]
    place = lax.broadcasted_iota(jnp.int32, lane_hot.shape[1:], 0)
    tall = lax.broadcasted_iota(jnp.int32, row_hot.shape[1:], 0)
    for k in range(count):
        spot = picks[k]
        lane_hot[k] = (place == spot % LANES).astype(jnp.float32).astype(jnp.bfloat16)
        row_hot[k] = (tall == spot // LANES).astype(jnp.float32).astype(jnp.bfloat16)


def finish_kernel(place, keep, pair, sent, other, basis, row_hot, lane_hot, disp_hbm, thermal_hbm, disp, thermal, shift,
                  left):
    sums = sent[pl.ds(0, SUB), :] + other[pl.ds(0, SUB), :]
    raw = [jnp.broadcast_to(jnp.sum(sums[k : k + 1, :], axis=1, keepdims=True), (1, LANES)) for k in range(8)]
    nu = [raw[0], raw[1]]
    for k in range(2, 7):
        nu.append(2.0 * raw[k] - raw[k % 2])
    nu.append(2.0 * raw[7] - nu[5] - 2.0 * raw[1])
    weights = coefficients(nu)
    wide = [jnp.broadcast_to(w, (SUB, LANES)) for w in weights]
    _, nx, _, nz = disp.shape
    tiles = nz // LANES
    depth = thermal.shape[1] // LANES
    fields = 3 * ITERS
    total = jnp.zeros((9 * depth, LANES), jnp.float32)
    odd = place[4]
    blocks = []
    for ref, offset, b, here in (
        (keep, 0, 1, 1),
        (pair, SUB, 2 - 2 * odd, jnp.where(odd == 1, place[2], place[3])),
        (other, SUB, 2 * odd, jnp.where(odd == 1, place[3], place[2])),
    ):
        valid = jnp.full((1, LANES), here, jnp.int32) == 1
        for a in range(3):
            pieces = []
            for c in range(3):
                value = None
                for j in range(ITERS):
                    term = weights[j] * ref[pl.ds(offset + a * fields + 3 * j + c, 1), :]
                    value = term if value is None else value + term
                value = jnp.where(valid, value, 0.0)
                for _ in range(3):
                    part = value.astype(jnp.bfloat16)
                    value = value - part.astype(jnp.float32)
                    pieces.append(row_hot[3 * a + b] * jnp.broadcast_to(part, (depth, LANES)))
            blocks.append((jnp.concatenate(pieces, axis=0), lane_hot[3 * a + b]))
            if len(blocks) == 2 or (ref is other and a == 2):
                wanted = jnp.concatenate([p for p, _ in blocks], axis=1)
                hot = jnp.concatenate([h for _, h in blocks], axis=1)
                total = total + lax.dot_general(wanted, hot, (((1,), (1,)), ((), ())),
                                                preferred_element_type=jnp.float32)
                blocks = []
    for c in range(3):
        whole = total[3 * c * depth : (3 * c + 1) * depth]
        whole = whole + total[(3 * c + 1) * depth : (3 * c + 2) * depth]
        shift[...] = whole + total[(3 * c + 2) * depth : (3 * c + 3) * depth]
        for r in range(depth):
            thermal[pl.ds(c, 1), pl.ds(r * LANES, LANES)] = shift[pl.ds(r, 1), :]
    copies = [pltpu.make_async_copy(thermal, thermal_hbm, left.at[0])]
    copies[0].start()

    def row(x, carry):
        for c in range(3):
            totals = []
            for t in range(tiles):
                at = pl.ds(pl.multiple_of(t * nx * SUB + x * SUB, SUB), SUB)
                total = wide[0] * basis[c, at, :]
                for j in range(1, 4):
                    total = total + wide[j] * basis[3 * j + c, at, :]
                totals.append(total)
            for t, total in enumerate(unmix(totals)):
                disp[c, x, :, pl.ds(t * LANES, LANES)] = total
        return carry

    half = nx // 2
    for k in range(2):
        at = pl.ds(k * half, half)
        lax.fori_loop(k * half, (k + 1) * half, row, 0)
        copies.append(pltpu.make_async_copy(disp.at[:, at], disp_hbm.at[:, at], left.at[1 + k]))
        copies[-1].start()
    for copy in copies:
        copy.wait()


def swap(last, leading, axis):
    peers = lax.axis_size(axis)
    up = [(i, i + 1) for i in range(peers - 1)]
    down = [(j, i) for i, j in up]
    return lax.ppermute(last, axis, up), lax.ppermute(leading, axis, down)


def after(value, *others):
    return lax.optimization_barrier((value, *others))[0]


def even_odd(axis):
    return [(i, i ^ 1) for i in range(lax.axis_size(axis))]


def odd_even(axis, around):
    peers = lax.axis_size(axis)
    pairs = [(i, i + 1 if i % 2 else i - 1) for i in range(peers)]
    return [(i, j % peers) for i, j in pairs if around or 0 <= j < peers]


def exchange(pair, other, axis):
    return lax.ppermute(pair, axis, even_odd(axis)), lax.ppermute(other, axis, odd_even(axis, False))


def far_hops(sums, axis):
    peers = lax.axis_size(axis)
    hop = peers // 2
    while hop >= 4:
        sums = sums + lax.ppermute(sums, axis, [(i, (i + hop) % peers) for i in range(peers)])
        hop //= 2
    return sums


def pair_hops(sums, pair, other, axis):
    pair = pair if sums is None else lax.dynamic_update_slice(pair, sums, (0, 0))
    pair_in = lax.ppermute(pair, axis, even_odd(axis))
    sent = lax.dynamic_update_slice(other, pair[:SUB] + pair_in[:SUB], (0, 0))
    return pair_in, sent, lax.ppermute(sent, axis, odd_even(axis, True))


def on_device(heat_level, emitting, holder, bucket, factors, rigidity, boundary, tally, accepting):
    f32, i32 = jnp.float32, jnp.int32
    ways = emitting.shape[1]
    per = emitting.shape[3] // LANES
    nx, ny, nz = rigidity.shape
    tiles = nz // LANES
    narrow = REACH - 2
    call = pl.pallas_call
    shape = jax.ShapeDtypeStruct
    dom, slab = lax.axis_index("dom"), lax.axis_index("slab")
    place = jnp.stack([dom > 0, dom < lax.axis_size("dom") - 1, slab > 0, slab < lax.axis_size("slab") - 1,
                       slab % 2, dom, dom % 2]).astype(i32)
    heat = heat_level.reshape(-1, LANES)
    emit_rows = emitting.reshape(-1, LANES)
    dom_message = shape((ways * per + narrow * tiles * ny, LANES), f32)
    third = shape((ways * per, LANES), i32)
    up, mixed = call(
        depart_kernel, out_shape=(dom_message, shape((nx, tiles * ny, LANES), f32)), in_specs=[HBM] * 3,
        out_specs=(VMEM,) * 2,
        scratch_shapes=[pltpu.VMEM(heat.shape, f32), pltpu.VMEM(third.shape, i32), pltpu.VMEM(rigidity.shape, f32),
                        pltpu.SemaphoreType.DMA((3,))],
        compiler_params=params(DEPART_MIB), cost_estimate=cost(5), name="depart",
    )(heat, emit_rows, rigidity)
    pairs_up = [(i, i + 1) for i in range(lax.axis_size("dom") - 1)]
    from_low = lax.ppermute(up, "dom", pairs_up)
    down = call(depart_down_kernel, out_shape=dom_message, in_specs=[VMEM] * 3, out_specs=VMEM,
                compiler_params=params(4), cost_estimate=cost(4), name="down")(heat, emit_rows, mixed)
    from_high = lax.ppermute(down, "dom", [(j, i) for i, j in pairs_up])
    near = call(near_kernel, out_shape=shape((ways * per, LANES), f32), in_specs=[VMEM] * 2, out_specs=VMEM,
                compiler_params=params(4), cost_estimate=cost(4), name="near")(after(heat, down), emit_rows)
    count = holder.size // LANES
    rows = ways * ways * per
    begun = call(
        functools.partial(plan_kernel, per), out_shape=shape((count, LANES), i32), in_specs=[SMEM, VMEM, VMEM],
        out_specs=VMEM,
        compiler_params=params(6), cost_estimate=cost(3), name="plan",
    )(place, after(holder, near), bucket)
    slab_message = shape((ways * per + tiles * wedge(nx, narrow)[1], LANES), f32)
    pair, other = call(
        forward_kernel, out_shape=(slab_message,) * 2, in_specs=[SMEM] + [VMEM] * 4, out_specs=(VMEM,) * 2,
        compiler_params=params(6), cost_estimate=cost(1), name="forward",
    )(place, from_low, after(near, begun), from_high, mixed)
    pair_in = lax.ppermute(pair, "slab", even_odd("slab"))
    keys, bounds = call(
        functools.partial(order_kernel, per), out_shape=(shape((count, LANES), i32), shape((SUB, LANES), i32)),
        in_specs=[SMEM, VMEM], out_specs=(VMEM, VMEM), compiler_params=params(6), cost_estimate=cost(3), name="order",
    )(place, after(begun, pair))
    other = after(other, keys, pair_in)
    other_in = lax.ppermute(other, "slab", odd_even("slab", False))
    early = call(
        early_kernel, out_shape=shape((count, LANES), f32), in_specs=[SMEM] + [VMEM] * 5 + [SMEM], out_specs=VMEM,
        scratch_shapes=[pltpu.VMEM((2 * ways * per, LANES), f32)], compiler_params=params(6), cost_estimate=cost(3),
        name="early",
    )(place, pair_in, from_low, near, from_high, keys, bounds)
    interp = call(
        pick_kernel, out_shape=shape((nx, tiles * ny, LANES), f32), in_specs=[SMEM] + [VMEM] * 7 + [SMEM, VMEM],
        out_specs=VMEM,
        scratch_shapes=[pltpu.VMEM((rows, LANES), f32), pltpu.VMEM((count, LANES), i32), pltpu.VMEM((count, LANES), f32)],
        compiler_params=params(8), cost_estimate=cost(12), name="pick",
    )(place, pair_in, other_in, from_low, near, from_high, keys, early, bounds, factors)
    p_low, p_high = swap(interp[nx - REACH :], interp[:REACH], "dom")
    halo = shape((tiles * wedge(nx, REACH)[1], LANES), f32)
    pair, other = call(pack_kernel, out_shape=(halo, halo), in_specs=[SMEM] + [VMEM] * 3,
                       out_specs=(VMEM, VMEM), compiler_params=params(6), cost_estimate=cost(1), name="pack",
                       )(place, p_low, interp, p_high)
    p_pair, p_other = exchange(pair, other, "slab")
    extent = nx + 2 * REACH
    field = pltpu.VMEM((3, tiles, extent, 3 * SUB, LANES), f32)
    basis, sums = call(
        krylov_kernel,
        out_shape=(shape((3 * ITERS, tiles * nx * ny, LANES), f32), shape((SUB, LANES), f32)),
        in_specs=[SMEM] + [VMEM] * 10,
        out_specs=(VMEM, VMEM),
        scratch_shapes=[pltpu.VMEM((tiles, extent, 3 * SUB, LANES), f32)] * 2 + [field] * 4,
        compiler_params=params(20), cost_estimate=cost(7), name="krylov",
    )(place, interp, p_low, p_high, p_pair, p_other, mixed, from_low, from_high, pair_in, other_in)
    sums = far_hops(sums, "dom")
    sums = far_hops(sums, "slab")
    fields = 3 * ITERS
    short = -(-ways * fields // SUB) * SUB
    kept, message = shape((short, LANES), f32), shape((SUB + short, LANES), f32)
    keep, pair, other = call(
        functools.partial(surface_kernel, nz), out_shape=(kept, message, message), in_specs=[SMEM, SMEM, VMEM, VMEM],
        out_specs=(VMEM,) * 3, scratch_shapes=[pltpu.VMEM((2 * SUB, LANES), i32), pltpu.VMEM((2 * SUB, LANES), f32)],
        compiler_params=params(6), cost_estimate=cost(4), name="surface",
    )(tally, place, basis, boundary.reshape(-1, 1, LANES))
    pair_in, sent, other_in = pair_hops(sums, pair, other, "dom")
    keep, pair, other = call(
        route_kernel, out_shape=(kept, message, message), in_specs=[SMEM] + [VMEM] * 4,
        out_specs=(VMEM,) * 3, compiler_params=params(4), cost_estimate=cost(1), name="route",
    )(place, keep, pair_in, sent, other_in)
    row_hot, lane_hot = call(
        hot_kernel, out_shape=(shape((ways * ways, heat.shape[0], LANES), jnp.bfloat16),
                               shape((ways * ways, LANES, LANES), jnp.bfloat16)),
        in_specs=[VMEM], out_specs=(VMEM, VMEM), compiler_params=params(4), cost_estimate=cost(1), name="hot",
    )(after(accepting, pair).reshape(-1, 1, LANES))
    pair_in = lax.ppermute(pair, "slab", even_odd("slab"))
    sent = lax.dynamic_update_slice(other, pair[:SUB] + pair_in[:SUB], (0, 0))
    other_in = lax.ppermute(sent, "slab", odd_even("slab", True))
    return call(
        finish_kernel,
        out_shape=(shape((3, nx, ny, nz), f32), shape((3, heat_level.shape[0]), f32)),
        in_specs=[SMEM] + [VMEM] * 7,
        out_specs=(HBM, HBM),
        scratch_shapes=[pltpu.VMEM((3, nx, ny, nz), f32), pltpu.VMEM((3, heat_level.shape[0]), f32),
                        pltpu.VMEM(heat.shape, f32), pltpu.SemaphoreType.DMA((3,))],
        compiler_params=params(8), cost_estimate=cost(2), name="finish",
    )(place, keep, pair_in, sent, other_in, basis, row_hot, lane_hot)


def solution(mesh):
    both = ("dom", "slab")
    in_specs = (
        P(both),
        P(both, None, None, None),
        P(None, "dom", "slab", None),
        P(None, "dom", "slab", None),
        P(None, "dom", "slab", None),
        P("dom", "slab", None),
        P(both, None, None, None),
        P(both, None),
        P(both, None, None, None),
    )
    out_specs = (P(None, "dom", "slab", None), P(None, both))

    return jax.shard_map(on_device, mesh=mesh, in_specs=in_specs, out_specs=out_specs, check_vma=False)
```

```python
import functools
import math

import jax
import jax.numpy as jnp
from jax import lax
from jax.experimental import pallas as pl
from jax.experimental.pallas import tpu as pltpu
from jax.sharding import PartitionSpec as P

ITERS = 4
COEF = 0.5
LANES = 128
CHUNK = 16
WEIGHT = 4e8
DEPART_MIB = 56
SUB = 8
CENTRE = 7.125
HALF = 6.875
REACH = ITERS + 1
VMEM = pl.BlockSpec(memory_space=pltpu.VMEM)
SMEM = pl.BlockSpec(memory_space=pltpu.SMEM)
HBM = pl.BlockSpec(memory_space=pltpu.HBM)


def params(mib):
    return pltpu.CompilerParams(vmem_limit_bytes=mib * 1024 * 1024)


def cost(micro, moved=0):
    return pl.CostEstimate(flops=int(micro * WEIGHT), bytes_accessed=moved, transcendentals=0)


def permute(value, lanes):
    return jnp.take_along_axis(value, lanes, axis=1, mode="promise_in_bounds")


def mix(values):
    tiles = len(values)
    lane = lax.broadcasted_iota(jnp.int32, values[0].shape, 1)
    share = LANES // tiles
    mixed = []
    for t in range(tiles):
        source = (lane * tiles + t) % LANES
        total = permute(values[0], source)
        for k in range(1, tiles):
            total = jnp.where(lane >= k * share, permute(values[k], source), total)
        mixed.append(total)
    return mixed


def unmix(values):
    tiles = len(values)
    lane = lax.broadcasted_iota(jnp.int32, values[0].shape, 1)
    share = LANES // tiles
    plain = []
    for k in range(tiles):
        source = k * share + lane // tiles
        total = permute(values[0], source)
        for t in range(1, tiles):
            total = jnp.where(lane % tiles == t, permute(values[t], source), total)
        plain.append(total)
    return plain


def wedge(nx, reach):
    rows, offset = [], 0
    for x in range(1 - reach, nx + reach - 1):
        width = reach - max(0, -x, x - nx + 1)
        rows.append((x, width, offset))
        offset += width
    return rows, offset


def lookup(table, first, rows, lanes, bits):
    if rows == 1:
        row = jnp.broadcast_to(table[pl.ds(first, 1), :], lanes.shape)
        return jnp.take_along_axis(row, lanes, axis=1, mode="promise_in_bounds")
    half = rows // 2
    lower = lookup(table, first, half, lanes, bits[:-1])
    upper = lookup(table, first + half, half, lanes, bits[:-1])
    return jnp.where(bits[-1], upper, lower)


def lookup_all(table, indices, chunk):
    rows = table.shape[0]
    depth = int(math.log2(chunk))
    lanes = [index & (LANES - 1) for index in indices]
    high = [index >> 7 for index in indices]
    outer = [value >> depth for value in high]

    def step(block, found):
        base = pl.multiple_of(block * chunk, chunk)
        fresh = []
        for lane, value, top, old in zip(lanes, high, outer, found):
            bits = [((value >> bit) & 1) == 1 for bit in range(depth)]
            fresh.append(jnp.where(top == block, lookup(table, base, chunk, lane, bits), old))
        return tuple(fresh)

    zero = jnp.zeros(indices[0].shape, jnp.float32)
    return lax.fori_loop(0, rows // chunk, step, tuple(zero for _ in indices))


def order2(a, b):
    if len(a) == 1:
        return (jnp.minimum(a[0], b[0]),), (jnp.maximum(a[0], b[0]),)
    swap = a[0] > b[0]
    low = [jnp.minimum(a[0], b[0])] + [jnp.where(swap, y, x) for x, y in zip(a[1:], b[1:])]
    high = [jnp.maximum(a[0], b[0])] + [jnp.where(swap, x, y) for x, y in zip(a[1:], b[1:])]
    return tuple(low), tuple(high)


def sublane_xor(value, mask):
    sub = lax.broadcasted_iota(jnp.int32, value.shape, 0)
    return jnp.take_along_axis(value, sub ^ mask, axis=0, mode="promise_in_bounds")


def keep_one(a, other, lower):
    if len(a) == 1:
        return (jnp.where(lower, jnp.minimum(a[0], other[0]), jnp.maximum(a[0], other[0])),)
    take = (a[0] > other[0]) == lower
    return tuple(jnp.where(take, y, x) for x, y in zip(a, other))


def sort_rows(refs, block, done=0, until=None):
    count = refs[0].shape[0] // SUB

    def load(v):
        at = pl.ds(pl.multiple_of(v * SUB, SUB), SUB)
        return tuple(r[at, :] for r in refs)

    def store(v, value):
        at = pl.ds(pl.multiple_of(v * SUB, SUB), SUB)
        for r, x in zip(refs, value): r[at, :] = x

    def strides(held, stride):
        while stride:
            for i in range(len(held)):
                if not i & stride:
                    held[i], held[i | stride] = order2(held[i], held[i | stride])
            stride //= 2

    def whole(t, carry):
        held = [load(t * block + i) for i in range(block)]
        size = 2
        while size <= block:
            for i in range(block):
                j = i ^ (size - 1)
                if i < j: held[i], held[j] = order2(held[i], held[j])
            strides(held, size // 4)
            size *= 2
        for i in range(block): store(t * block + i, held[i])
        return carry

    def finish(t, carry):
        held = [load(t * block + i) for i in range(block)]
        strides(held, block // 2)
        for i in range(block): store(t * block + i, held[i])
        return carry

    if not done:
        lax.fori_loop(0, count // block, whole, 0, unroll=2)
    size = 2 * max(done, block)
    while size <= (until or count * SUB):
        span = min(size, count)
        flip = size // count - 1 if size > count else 0
        groups = span // block

        def top(t, carry):
            base = (t // (block // 2)) * span
            i = t % (block // 2)
            spots = []
            for j in range(groups):
                spots += [base + i + block * j, base + block - 1 - i + block * j]
            held = [load(v) for v in spots]
            n = len(held)
            if flip:
                sub = lax.broadcasted_iota(jnp.int32, (SUB, LANES), 0)
                lower = (sub & ((flip + 1) // 2)) == 0
                turned = [tuple(sublane_xor(x, flip) for x in h) for h in held]
                held = [keep_one(held[k], turned[n - 1 - k], lower) for k in range(n)]
                bit = (flip + 1) // 4
                while bit:
                    lower = (sub & bit) == 0
                    held = [keep_one(h, tuple(sublane_xor(x, bit) for x in h), lower) for h in held]
                    bit //= 2
                far = groups // 2
            else:
                for k in range(n // 2):
                    held[k], held[n - 1 - k] = order2(held[k], held[n - 1 - k])
                far = groups // 4
            while far:
                for j in range(groups):
                    if not j & far:
                        for side in range(2):
                            x, y = 2 * j + side, 2 * (j | far) + side
                            held[x], held[y] = order2(held[x], held[y])
                far //= 2
            for v, h in zip(spots, held): store(v, h)
            return carry

        lax.fori_loop(0, (count // span) * (block // 2), top, 0, unroll=max(1, 16 // groups))
        lax.fori_loop(0, count // block, finish, 0, unroll=2)
        size *= 2


def blocks_of(place):
    kinds = 1 + place[0] + place[1]
    return kinds, 1 - place[0], 2 - place[4], 1 + place[4]


def plan_kernel(per, place, shift, bucket, keys):
    kinds, first, left, right = blocks_of(place)
    corners, nx, _, nz = shift.shape
    tiles = nz // LANES
    count = corners * nx * tiles
    sub = lax.broadcasted_iota(jnp.int32, (SUB, LANES), 0)

    def build(x, carry):
        for c in range(corners):
            for t in range(tiles):
                at = pl.ds(t * LANES, LANES)
                way = shift[c, x, :, at]
                a = (way * 11) >> 5
                b = way - 3 * a
                block = jnp.where(b == 1, 0, jnp.where(b == 0, left * kinds, right * kinds)) + (a - first)
                flat = block * (per * LANES) + bucket[c, x, :, at]
                if c:
                    flat = pltpu.roll(flat, c * (LANES // corners), axis=1)
                v = (c * nx + x) * tiles + t
                keys[pl.ds(pl.multiple_of(v * SUB, SUB), SUB), :] = flat * (count * SUB) + (sub * count + v)
        return carry

    lax.fori_loop(0, nx, build, 0, unroll=2)
    sort_rows([keys], 32, until=count)


def order_kernel(per, place, begun, keys, bounds):
    keys[...] = begun[...]
    count = keys.shape[0] // SUB
    sort_rows([keys], 32, done=count)
    low_bits = int(math.log2(count * SUB * LANES))
    lane = lax.broadcasted_iota(jnp.int32, (SUB, LANES), 1)
    base = jnp.zeros((SUB, LANES), jnp.float32)
    width = jnp.zeros((SUB, 1), jnp.float32)
    top = jnp.zeros((SUB, 1), jnp.float32)
    for g in range(count // SUB):
        least = (keys[pl.ds(g * SUB * SUB, SUB), :] >> low_bits).astype(jnp.float32)
        most = (keys[pl.ds(g * SUB * SUB + SUB * (SUB - 1), SUB), :] >> low_bits).astype(jnp.float32)
        least = jnp.min(least, axis=1, keepdims=True)
        most = jnp.max(most, axis=1, keepdims=True)
        base = jnp.where(lane == g, least, base)
        width = jnp.maximum(width, most - least + 1.0)
        top = jnp.maximum(top, most)
    trips = (width.astype(jnp.int32) + (CHUNK - 1)) // CHUNK
    ready = 2 * blocks_of(place)[0] * per
    rows = jnp.where(top.astype(jnp.int32) < ready, ready, 9 * per)
    start = jnp.minimum(base.astype(jnp.int32), rows - trips * CHUNK)
    latest = jnp.max(jnp.where(lane < count // SUB, start, 0).astype(jnp.float32), axis=1, keepdims=True)
    soon = jnp.clip((ready - latest.astype(jnp.int32)) // CHUNK, 0, trips)
    bounds[...] = jnp.where(lane == LANES - 1, trips, jnp.where(lane == LANES - 2, soon, start))


def visit(table, keys, bounds, soon, before, store):
    count = keys.shape[0] // SUB
    pos_bits = int(math.log2(count * SUB))
    depth = int(math.log2(CHUNK))
    per = count // SUB

    def body(s, carry):
        own = [keys[pl.ds(SUB * SUB * g + s, SUB, stride=SUB), :] for g in range(per)]
        start = [bounds[s, g] for g in range(per)]

        def step(n, found):
            fresh = []
            for g in range(per):
                lanes = (own[g] >> pos_bits) & (LANES - 1)
                first = start[g] + n * CHUNK
                rel = (own[g] >> (pos_bits + 7)) - first
                bits = [((rel >> b) & 1) == 1 for b in range(depth)]
                fresh.append(jnp.where((rel >> depth) == 0, lookup(table, first, CHUNK, lanes, bits), found[g]))
            return tuple(fresh)

        spots = [pl.ds(SUB * SUB * g + s, SUB, stride=SUB) for g in range(per)]
        least = 0 if soon else bounds[s, LANES - 2]
        most = bounds[s, LANES - 2 if soon else LANES - 1]
        found = lax.fori_loop(least, most, step, tuple(before(at) for at in spots))
        for g, at in enumerate(spots):
            store(at, found[g], own[g] & (count * SUB - 1))
        return carry

    lax.fori_loop(0, SUB, body, 0)


def slots_of(heat, picks, first, out, rows):
    group = SUB * SUB

    def body(g, carry):
        base = pl.multiple_of(g * group, group)
        found = lookup_all(heat, [picks[pl.ds(first + base + SUB * k, SUB), :] for k in range(SUB)], heat.shape[0])
        for k in range(SUB):
            out[pl.ds(base + SUB * k, SUB), :] = found[k]
        return carry

    lax.fori_loop(0, rows // group, body, 0)


def depart_kernel(heat_hbm, picks_hbm, rigid_hbm, up, heat, picks, rigid, arrived):
    rows, narrow = picks.shape[0], rigid.shape[0]
    sources = (rigid_hbm.at[pl.ds(rigid_hbm.shape[0] - narrow, narrow)], heat_hbm,
               picks_hbm.at[pl.ds(picks_hbm.shape[0] - rows, rows), :])
    copies = [
        pltpu.make_async_copy(source, target, arrived.at[k])
        for k, (source, target) in enumerate(zip(sources, (rigid, heat, picks)))
    ]
    for copy in copies:
        copy.start()
    tiles = rigid.shape[2] // LANES
    copies[0].wait()
    for x in range(narrow):
        for t, value in enumerate(mix([rigid[x, :, pl.ds(t * LANES, LANES)] for t in range(tiles)])):
            up[pl.ds(rows + (x * tiles + t) * SUB, SUB), :] = value
    copies[1].wait()
    copies[2].wait()
    slots_of(heat, picks, 0, up, rows)


def depart_down_kernel(heat, picks, rigid, down, mixed):
    narrow = REACH - 2
    nx, _, nz = rigid.shape
    tiles = nz // LANES
    rows = down.shape[0] - narrow * tiles * SUB
    for x in range(nx):
        for t, value in enumerate(mix([rigid[x, :, pl.ds(t * LANES, LANES)] for t in range(tiles)])):
            mixed[x, pl.ds(t * SUB, SUB), :] = value
            if x < narrow:
                down[pl.ds(rows + (x * tiles + t) * SUB, SUB), :] = value
    slots_of(heat, picks, 0, down, rows)


def near_kernel(heat, picks, near):
    slots_of(heat, picks, near.shape[0], near, near.shape[0])


def forward_kernel(place, low, near, high, rigid, pair, other):
    nx, ny = rigid.shape[0], SUB
    per = near.shape[0] // 3
    tiles = rigid.shape[1] // SUB
    odd = place[4] == 1
    rows, size = wedge(nx, REACH - 2)

    def give(to, up, down):
        pair[to, :] = jnp.where(odd, down, up)
        other[to, :] = jnp.where(odd, up, down)

    for a, ref in enumerate((low, near, high)):
        give(pl.ds(a * per, per), ref[pl.ds(2 * per, per), :], ref[pl.ds(0, per), :])
    for t in range(tiles):
        for x, width, offset in rows:
            to = pl.ds(3 * per + t * size + offset, width)
            if 0 <= x < nx:
                base = t * SUB
                give(to, rigid[x, pl.ds(base + ny - width, width), :], rigid[x, pl.ds(base, width), :])
            else:
                ref, k = (low, x + REACH - 2) if x < 0 else (high, x - nx)
                base = 3 * per + (k * tiles + t) * SUB
                give(to, ref[pl.ds(base + ny - width, width), :], ref[pl.ds(base, width), :])


def lay(table, per, place, columns):
    kinds, first = blocks_of(place)[:2]
    for valid, column, readers in columns:
        for a, read in enumerate(readers):
            here = valid if a == 1 else jnp.logical_and(valid, place[0 if a == 0 else 1] == 1)

            @pl.when(here)
            def _():
                row = pl.multiple_of((column * kinds + a - first) * per, per)
                table[pl.ds(row, per), :] = read()


def early_kernel(place, pair, low, near, high, keys, bounds, value, table):
    per = near.shape[0] // 3
    own = [lambda ref=ref: ref[pl.ds(per, per), :] for ref in (low, near, high)]
    side = [lambda at=pl.ds(a * per, per): pair[at, :] for a in range(3)]
    lay(table, per, place, [(place[0] >= 0, 0, own), (place[0] >= 0, 1, side)])

    def store(at, found, spot):
        value[at, :] = found

    visit(table, keys, bounds, True, lambda at: jnp.zeros((SUB, LANES), jnp.float32), store)


def pick_kernel(place, pair, other, low, near, high, keys, early, bounds, factor, out, table, position, value):
    odd = place[4] == 1
    corners, nx, _, nz = factor.shape
    tiles = nz // LANES
    slots = near.shape[0] // 3
    own = [lambda ref=ref: ref[pl.ds(slots, slots), :] for ref in (low, near, high)]

    def side(even_ref, odd_ref):
        return [lambda at=pl.ds(a * slots, slots): jnp.where(odd, odd_ref[at, :], even_ref[at, :]) for a in range(3)]

    _, _, left, right = blocks_of(place)
    lay(table, slots, place, [(place[0] >= 0, 0, own), (place[2] == 1, left, side(other, pair)),
                              (place[3] == 1, right, side(pair, other))])

    def store(at, found, spot):
        value[at, :] = found
        position[at, :] = spot

    visit(table, keys, bounds, False, lambda at: early[at, :], store)
    sort_rows([position, value], 16)

    def blend(x, carry):
        blended = []
        for t in range(tiles):
            at = pl.ds(t * LANES, LANES)
            total = None
            for c in range(corners):
                v = (c * nx + x) * tiles + t
                got = value[pl.ds(pl.multiple_of(v * SUB, SUB), SUB), :]
                if c:
                    got = pltpu.roll(got, LANES - c * (LANES // corners), axis=1)
                got = factor[c, x, :, at] * got
                total = got if total is None else total + got
            blended.append(total)
        for t, total in enumerate(mix(blended)):
            out[x, pl.ds(t * SUB, SUB), :] = total
        return carry

    lax.fori_loop(0, nx, blend, 0, unroll=2)


def pack_kernel(place, low, own, high, pair, other):
    nx, ny = own.shape[0], SUB
    tiles = own.shape[1] // SUB
    odd = place[4] == 1
    rows, size = wedge(nx, REACH)
    for t in range(tiles):
        for x, width, offset in rows:
            ref, k = (own, x) if 0 <= x < nx else (low, x + REACH) if x < 0 else (high, x - nx)
            up = ref[k, pl.ds(t * SUB + ny - width, width), :]
            down = ref[k, pl.ds(t * SUB, width), :]
            to = pl.ds(t * size + offset, width)
            pair[to, :] = jnp.where(odd, down, up)
            other[to, :] = jnp.where(odd, up, down)


def unpack(target, reach, own, dom_low, dom_high, pair, other, offset, odd, change):
    nx = own.shape[0]
    tiles = own.shape[1] // SUB
    rows, size = wedge(nx, reach)
    for t in range(tiles):
        for x in range(-reach, nx + reach):
            if 0 <= x < nx:
                mine = own[x, pl.ds(t * SUB, SUB), :]
            else:
                mine = dom_low(x + reach, t) if x < 0 else dom_high(x - nx, t)
            target[t, REACH + x, pl.ds(SUB, SUB), :] = change(mine, REACH + x, 1)
        for x, width, row in rows:
            at = pl.ds(offset + t * size + row, width)
            even_low, odd_low = other[at, :], pair[at, :]
            target[t, REACH + x, pl.ds(SUB - width, width), :] = change(jnp.where(odd, odd_low, even_low), REACH + x, 0)
            target[t, REACH + x, pl.ds(2 * SUB, width), :] = change(jnp.where(odd, even_low, odd_low), REACH + x, 2)


def krylov_kernel(inside, own, p_low, p_high, p_pair, p_other, rigid, d_low, d_high, d_pair, d_other,
                  basis, sums, temp, diag, u0, u1, u2, u3):
    nx = own.shape[0]
    tiles = own.shape[1] // SUB
    parts = temp.shape[2] // SUB
    held = (u0, u1, u2, u3)
    flag = [inside[k].astype(jnp.float32) for k in range(4)]

    def mask(x, part):
        at_x = jnp.where(x < REACH, flag[0], jnp.where(x >= REACH + nx, flag[1], 1.0))
        return at_x * (flag[2] if part == 0 else flag[3] if part == 2 else 1.0)

    temp[...] = jnp.zeros_like(temp)
    odd = inside[4] == 1
    base = d_pair.shape[0] - tiles * wedge(nx, REACH - 2)[1]
    first_d = d_low.shape[0] - tiles * SUB * (REACH - 2)

    def plane(ref):
        return lambda x, t: ref[x, pl.ds(t * SUB, SUB), :]

    def message(ref):
        return lambda x, t: ref[pl.ds(first_d + (x * tiles + t) * SUB, SUB), :]

    unpack(temp, REACH, own, plane(p_low), plane(p_high), p_pair, p_other, 0, odd, lambda v, x, part: v)
    diag[...] = jnp.zeros_like(diag)
    unpack(diag, REACH - 2, rigid, message(d_low), message(d_high), d_pair, d_other, base, odd,
           lambda v, x, part: (v * (2.0 / HALF) + 2.0 * (6.0 - CENTRE) / HALF) * mask(x, part))
    lane = lax.broadcasted_iota(jnp.int32, (SUB, LANES), 1)
    first, last = lane == 0, lane == LANES - 1
    zero = jnp.zeros((SUB, LANES), jnp.float32)

    def around_z(values):
        back = jnp.where(first, zero, pltpu.roll(values[-1], 1, axis=1))
        ahead = jnp.where(last, zero, pltpu.roll(values[0], LANES - 1, axis=1))
        return [(values[t - 1] if t else back, values[t + 1] if t + 1 < tiles else ahead) for t in range(tiles)]

    def around_y(ref, head, x, part):
        base = part * SUB
        mine = ref[(*head, x, pl.ds(base, SUB))]
        below = pltpu.roll(mine, 1, axis=0) if part == 0 else ref[(*head, x, pl.ds(base - 1, SUB))]
        above = pltpu.roll(mine, SUB - 1, axis=0) if part == parts - 1 else ref[(*head, x, pl.ds(base + 1, SUB))]
        return mine, below, above

    def load_row(x, carry):
        for part in range(parts):
            scale = COEF * mask(x, part)
            rows = [around_y(temp, (t,), x, part) for t in range(tiles)]
            along = around_z([r[0] for r in rows])
            for t in range(tiles):
                ahead = temp[t, x + 1, pl.ds(part * SUB, SUB), :]
                back = temp[t, x - 1, pl.ds(part * SUB, SUB), :]
                u0[0, t, x, pl.ds(part * SUB, SUB), :] = scale * (ahead - back)
                u0[1, t, x, pl.ds(part * SUB, SUB), :] = scale * (rows[t][2] - rows[t][1])
                u0[2, t, x, pl.ds(part * SUB, SUB), :] = scale * (along[t][1] - along[t][0])
        return carry

    lax.fori_loop(1, nx + 2 * REACH - 1, load_row, 0, unroll=2)

    def twice(ref, c, x, part):
        coefficient = (2.0 / HALF) * mask(x, part)
        rows = [around_y(ref, (c, t), x, part) for t in range(tiles)]
        along = around_z([r[0] for r in rows])
        results = []
        for t in range(tiles):
            near = rows[t][1] + rows[t][2] + along[t][0] + along[t][1]
            near = near + ref[c, t, x + 1, pl.ds(part * SUB, SUB), :] + ref[c, t, x - 1, pl.ds(part * SUB, SUB), :]
            results.append(diag[t, x, pl.ds(part * SUB, SUB), :] * rows[t][0] - coefficient * near)
        return results, [r[0] for r in rows]

    for order in range(1, ITERS):
        source, target = held[order - 1], held[order]

        def apply_row(x, carry):
            for c in range(3):
                for part in range(parts):
                    doubled, _ = twice(source, c, x, part)
                    for t in range(tiles):
                        at = (c, t, x, pl.ds(part * SUB, SUB))
                        if order == 1:
                            target[at] = 0.5 * doubled[t]
                        else:
                            target[at] = doubled[t] - held[order - 2][at]
            return carry

        margin = ITERS - order
        lax.fori_loop(REACH - margin, REACH + nx + margin, apply_row, 0, unroll=2)

    def dots_row(x, carry):
        carry = list(carry)
        for c in range(3):
            doubled, u = twice(u3, c, REACH + x, 1)
            for t in range(tiles):
                at = (c, t, REACH + x, pl.ds(SUB, SUB))
                v = [u0[at], u1[at], u2[at], u[t]]
                pairs = [(v[0], v[0]), (v[0], v[1]), (v[1], v[1]), (v[1], v[2]), (v[2], v[2]), (v[2], v[3]),
                         (v[3], v[3]), (v[3], doubled[t])]
                for k, (left, right) in enumerate(pairs):
                    carry[k] = carry[k] + left * right
                for j in range(4):
                    basis[3 * j + c, pl.ds(pl.multiple_of(t * nx * SUB + x * SUB, SUB), SUB), :] = v[j]
        return tuple(carry)

    totals = lax.fori_loop(0, nx, dots_row, tuple(zero for _ in range(8)), unroll=2)
    for k in range(8):
        sums[pl.ds(k, 1), :] = jnp.sum(totals[k], axis=0, keepdims=True)


def surface_kernel(nz, tally, place, basis, picks, keep, pair, other, index, live):
    fields, rows, _ = basis.shape
    count = picks.shape[0]
    tiles = nz // LANES
    block = rows // tiles
    odd = place[6] == 1
    lane = lax.broadcasted_iota(jnp.int32, (1, LANES), 1)
    sub = lax.broadcasted_iota(jnp.int32, (SUB, LANES), 0)
    for k in range(count):
        spot = picks[k]
        along = spot % nz
        index[pl.ds(k, 1), :] = ((along % tiles) * block + spot // nz) * LANES + along // tiles
        live[pl.ds(k, 1), :] = (lane < tally[0, k]).astype(jnp.float32)

    def give(f, values):
        for b in range(3):
            keep[pl.ds(b * fields + f, 1), :] = values[3 + b]
            to = pl.ds(SUB + b * fields + f, 1)
            pair[to, :] = jnp.where(odd, values[b], values[6 + b])
            other[to, :] = jnp.where(odd, values[6 + b], values[b])

    depth = int(math.log2(rows))

    def body(f, carry):
        table = basis.at[f]
        spots = index[pl.ds(0, SUB), :]
        high = spots >> 7
        bits = [((high >> bit) & 1) == 1 for bit in range(depth)]
        found = lookup(table, 0, rows, spots & (LANES - 1), bits)
        found = jnp.where(live[pl.ds(0, SUB), :] > 0.5, found, 0.0)
        values = [found[k : k + 1, :] for k in range(SUB)]
        for k in range(SUB, count):
            spots = jnp.broadcast_to(index[pl.ds(k, 1), :], (SUB, LANES))
            lanes, high = spots & (LANES - 1), spots >> 7
            total = jnp.zeros((SUB, LANES), jnp.float32)
            for g in range(0, rows, SUB):
                got = jnp.take_along_axis(table[pl.ds(g, SUB), :], lanes, axis=1, mode="promise_in_bounds")
                total = jnp.where(high == sub + g, got, total)
            total = jnp.sum(total, axis=0, keepdims=True)
            total = jnp.where(live[pl.ds(k, 1), :] > 0.5, total, 0.0)
            values.append(total)
        give(f, values)
        return carry

    lax.fori_loop(0, fields, body, 0, unroll=3)


def route_kernel(place, kept, pair_in, sent, other_in, keep, pair, other):
    fields = 3 * ITERS
    pair[pl.ds(0, SUB), :] = sent[pl.ds(0, SUB), :] + other_in[pl.ds(0, SUB), :]
    odd, odd_dom = place[4] == 1, place[6] == 1
    for b in range(3):
        at = pl.ds(SUB + b * fields, fields)
        one, two = pair_in[at, :], other_in[at, :]
        low = jnp.where(odd_dom, one, two) * place[0].astype(jnp.float32)
        high = jnp.where(odd_dom, two, one) * place[1].astype(jnp.float32)
        for a, rows in ((0, low), (1, kept[pl.ds(b * fields, fields), :]), (2, high)):
            if b == 1:
                keep[pl.ds(a * fields, fields), :] = rows
            else:
                to = pl.ds(SUB + a * fields, fields)
                chosen = odd if b == 0 else jnp.logical_not(odd)

                @pl.when(chosen)
                def _():
                    pair[to, :] = rows

                @pl.when(jnp.logical_not(chosen))
                def _():
                    other[to, :] = rows


def coefficients(nu):
    half = 0.5

    def gram(i, j):
        return half * (nu[i + j] + nu[abs(i - j)])

    def inner(i, j):
        if j == 0:
            return gram(i, 1)
        return half * (gram(i, j + 1) + gram(i, j - 1))

    def form(vector, matrix):
        n = len(vector)
        total = None
        for i in range(n):
            for j in range(i, n):
                term = vector[i] * vector[j] * matrix(i, j)
                term = term if i == j else 2.0 * term
                total = term if total is None else total + term
        return total

    one = jnp.ones_like(nu[0])
    found, residual, direction = [], [one], [one]
    rr = nu[0]
    for iteration in range(ITERS):
        energy = form(direction, lambda i, j: CENTRE * gram(i, j) + HALF * inner(i, j))
        alpha = rr / energy
        found = [
            (found[i] if i < len(found) else 0.0) + alpha * direction[i] for i in range(len(direction))
        ]
        if iteration + 1 == ITERS:
            break
        image = [CENTRE * d for d in direction] + [jnp.zeros_like(one)]
        for j, d in enumerate(direction):
            if j == 0:
                image[1] = image[1] + HALF * d
            else:
                image[j + 1] = image[j + 1] + half * HALF * d
                image[j - 1] = image[j - 1] + half * HALF * d
        residual = residual + [jnp.zeros_like(one)]
        residual = [r - alpha * w for r, w in zip(residual, image)]
        fresh = form(residual, gram)
        ratio = fresh / rr
        direction = direction + [jnp.zeros_like(one)]
        direction = [r + ratio * d for r, d in zip(residual, direction)]
        rr = fresh
    return found


def plain_kernel(basis, plain):
    fields, nx, _, nz = plain.shape
    tiles = nz // LANES

    def row(x, carry):
        for f in range(fields):
            at = [pl.ds(pl.multiple_of(t * nx * SUB + x * SUB, SUB), SUB) for t in range(tiles)]
            for t, value in enumerate(unmix([basis[f, k, :] for k in at])):
                plain[f, x, :, pl.ds(t * LANES, LANES)] = value
        return carry

    lax.fori_loop(0, nx, row, 0)


def hot_kernel(picks, row_hot, lane_hot):
    count = picks.shape[0]
    place = lax.broadcasted_iota(jnp.int32, lane_hot.shape[1:], 0)
    tall = lax.broadcasted_iota(jnp.int32, row_hot.shape[1:], 0)
    for k in range(count):
        spot = picks[k]
        lane_hot[k] = (place == spot % LANES).astype(jnp.float32).astype(jnp.bfloat16)
        row_hot[k] = (tall == spot // LANES).astype(jnp.float32).astype(jnp.bfloat16)


def finish_kernel(place, keep, pair, sent, other, basis, row_hot, lane_hot, disp_hbm, thermal_hbm, disp, thermal, shift,
                  left):
    sums = sent[pl.ds(0, SUB), :] + other[pl.ds(0, SUB), :]
    raw = [jnp.broadcast_to(jnp.sum(sums[k : k + 1, :], axis=1, keepdims=True), (1, LANES)) for k in range(8)]
    nu = [raw[0], raw[1]]
    for k in range(2, 7):
        nu.append(2.0 * raw[k] - raw[k % 2])
    nu.append(2.0 * raw[7] - nu[5] - 2.0 * raw[1])
    weights = coefficients(nu)
    wide = [jnp.broadcast_to(w, (SUB, LANES)) for w in weights]
    _, nx, _, nz = disp.shape
    tiles = nz // LANES
    depth = thermal.shape[1] // LANES
    fields = 3 * ITERS
    total = jnp.zeros((9 * depth, LANES), jnp.float32)
    odd = place[4]
    blocks = []
    for ref, offset, b, here in (
        (keep, 0, 1, 1),
        (pair, SUB, 2 - 2 * odd, jnp.where(odd == 1, place[2], place[3])),
        (other, SUB, 2 * odd, jnp.where(odd == 1, place[3], place[2])),
    ):
        valid = jnp.full((1, LANES), here, jnp.int32) == 1
        for a in range(3):
            pieces = []
            for c in range(3):
                value = None
                for j in range(ITERS):
                    term = weights[j] * ref[pl.ds(offset + a * fields + 3 * j + c, 1), :]
                    value = term if value is None else value + term
                value = jnp.where(valid, value, 0.0)
                for _ in range(3):
                    part = value.astype(jnp.bfloat16)
                    value = value - part.astype(jnp.float32)
                    pieces.append(row_hot[3 * a + b] * jnp.broadcast_to(part, (depth, LANES)))
            blocks.append((jnp.concatenate(pieces, axis=0), lane_hot[3 * a + b]))
            if len(blocks) == 2 or (ref is other and a == 2):
                wanted = jnp.concatenate([p for p, _ in blocks], axis=1)
                hot = jnp.concatenate([h for _, h in blocks], axis=1)
                total = total + lax.dot_general(wanted, hot, (((1,), (1,)), ((), ())),
                                                preferred_element_type=jnp.float32)
                blocks = []
    for c in range(3):
        whole = total[3 * c * depth : (3 * c + 1) * depth]
        whole = whole + total[(3 * c + 1) * depth : (3 * c + 2) * depth]
        shift[...] = whole + total[(3 * c + 2) * depth : (3 * c + 3) * depth]
        for r in range(depth):
            thermal[pl.ds(c, 1), pl.ds(r * LANES, LANES)] = shift[pl.ds(r, 1), :]
    copies = [pltpu.make_async_copy(thermal, thermal_hbm, left.at[0])]
    copies[0].start()

    def row(x, carry):
        for c in range(3):
            for t in range(tiles):
                at = pl.ds(t * LANES, LANES)
                total = wide[0] * basis[c, x, :, at]
                for j in range(1, 4):
                    total = total + wide[j] * basis[3 * j + c, x, :, at]
                disp[c, x, :, at] = total
        return carry

    half = nx // 2
    for k in range(2):
        at = pl.ds(k * half, half)
        lax.fori_loop(k * half, (k + 1) * half, row, 0)
        copies.append(pltpu.make_async_copy(disp.at[:, at], disp_hbm.at[:, at], left.at[1 + k]))
        copies[-1].start()
    for copy in copies:
        copy.wait()


def swap(last, leading, axis):
    peers = lax.axis_size(axis)
    up = [(i, i + 1) for i in range(peers - 1)]
    down = [(j, i) for i, j in up]
    return lax.ppermute(last, axis, up), lax.ppermute(leading, axis, down)


def after(value, *others):
    return lax.optimization_barrier((value, *others))[0]


def even_odd(axis):
    return [(i, i ^ 1) for i in range(lax.axis_size(axis))]


def odd_even(axis, around):
    peers = lax.axis_size(axis)
    pairs = [(i, i + 1 if i % 2 else i - 1) for i in range(peers)]
    return [(i, j % peers) for i, j in pairs if around or 0 <= j < peers]


def exchange(pair, other, axis):
    return lax.ppermute(pair, axis, even_odd(axis)), lax.ppermute(other, axis, odd_even(axis, False))


def far_hops(sums, axis):
    peers = lax.axis_size(axis)
    hop = peers // 2
    while hop >= 4:
        sums = sums + lax.ppermute(sums, axis, [(i, (i + hop) % peers) for i in range(peers)])
        hop //= 2
    return sums


def pair_hops(sums, pair, other, axis):
    pair = pair if sums is None else lax.dynamic_update_slice(pair, sums, (0, 0))
    pair_in = lax.ppermute(pair, axis, even_odd(axis))
    sent = lax.dynamic_update_slice(other, pair[:SUB] + pair_in[:SUB], (0, 0))
    other_in = lax.ppermute(sent, axis, odd_even(axis, True))
    return pair_in, sent, other_in


def on_device(heat_level, emitting, holder, bucket, factors, rigidity, boundary, tally, accepting):
    f32, i32 = jnp.float32, jnp.int32
    ways = emitting.shape[1]
    per = emitting.shape[3] // LANES
    nx, ny, nz = rigidity.shape
    tiles = nz // LANES
    narrow = REACH - 2
    call = pl.pallas_call
    shape = jax.ShapeDtypeStruct
    dom, slab = lax.axis_index("dom"), lax.axis_index("slab")
    place = jnp.stack([dom > 0, dom < lax.axis_size("dom") - 1, slab > 0, slab < lax.axis_size("slab") - 1,
                       slab % 2, dom, dom % 2]).astype(i32)
    heat = heat_level.reshape(-1, LANES)
    emit_rows = emitting.reshape(-1, LANES)
    dom_message = shape((ways * per + narrow * tiles * ny, LANES), f32)
    third = shape((ways * per, LANES), i32)
    up = call(
        depart_kernel, out_shape=dom_message, in_specs=[HBM] * 3, out_specs=VMEM,
        scratch_shapes=[pltpu.VMEM(heat.shape, f32), pltpu.VMEM(third.shape, i32), pltpu.VMEM((narrow, ny, nz), f32),
                        pltpu.SemaphoreType.DMA((3,))],
        compiler_params=params(DEPART_MIB), cost_estimate=cost(5), name="depart",
    )(heat, emit_rows, rigidity)
    pairs_up = [(i, i + 1) for i in range(lax.axis_size("dom") - 1)]
    from_low = lax.ppermute(up, "dom", pairs_up)
    down, mixed = call(
        depart_down_kernel, out_shape=(dom_message, shape((nx, tiles * ny, LANES), f32)), in_specs=[VMEM] * 3,
        out_specs=(VMEM,) * 2, compiler_params=params(4), cost_estimate=cost(4), name="down",
    )(after(heat, up), emit_rows, rigidity)
    from_high = lax.ppermute(down, "dom", [(j, i) for i, j in pairs_up])
    near = call(near_kernel, out_shape=shape((ways * per, LANES), f32), in_specs=[VMEM] * 2, out_specs=VMEM,
                compiler_params=params(4), cost_estimate=cost(4), name="near")(after(heat, down), emit_rows)
    count = holder.size // LANES
    rows = ways * ways * per
    begun = call(
        functools.partial(plan_kernel, per), out_shape=shape((count, LANES), i32), in_specs=[SMEM, VMEM, VMEM],
        out_specs=VMEM,
        compiler_params=params(6), cost_estimate=cost(3), name="plan",
    )(place, after(holder, near), bucket)
    slab_message = shape((ways * per + tiles * wedge(nx, narrow)[1], LANES), f32)
    pair, other = call(
        forward_kernel, out_shape=(slab_message,) * 2, in_specs=[SMEM] + [VMEM] * 4, out_specs=(VMEM,) * 2,
        compiler_params=params(6), cost_estimate=cost(1), name="forward",
    )(place, from_low, after(near, begun), from_high, mixed)
    pair_in = lax.ppermute(pair, "slab", even_odd("slab"))
    keys, bounds = call(
        functools.partial(order_kernel, per), out_shape=(shape((count, LANES), i32), shape((SUB, LANES), i32)),
        in_specs=[SMEM, VMEM], out_specs=(VMEM, VMEM), compiler_params=params(6), cost_estimate=cost(3), name="order",
    )(place, after(begun, pair))
    other = after(other, keys, pair_in)
    other_in = lax.ppermute(other, "slab", odd_even("slab", False))
    early = call(
        early_kernel, out_shape=shape((count, LANES), f32), in_specs=[SMEM] + [VMEM] * 5 + [SMEM], out_specs=VMEM,
        scratch_shapes=[pltpu.VMEM((2 * ways * per, LANES), f32)], compiler_params=params(6), cost_estimate=cost(3),
        name="early",
    )(place, pair_in, from_low, near, from_high, keys, bounds)
    interp = call(
        pick_kernel, out_shape=shape((nx, tiles * ny, LANES), f32), in_specs=[SMEM] + [VMEM] * 7 + [SMEM, VMEM],
        out_specs=VMEM,
        scratch_shapes=[pltpu.VMEM((rows, LANES), f32), pltpu.VMEM((count, LANES), i32), pltpu.VMEM((count, LANES), f32)],
        compiler_params=params(8), cost_estimate=cost(12), name="pick",
    )(place, pair_in, other_in, from_low, near, from_high, keys, early, bounds, factors)
    p_low, p_high = swap(interp[nx - REACH :], interp[:REACH], "dom")
    halo = shape((tiles * wedge(nx, REACH)[1], LANES), f32)
    pair, other = call(pack_kernel, out_shape=(halo, halo), in_specs=[SMEM] + [VMEM] * 3,
                       out_specs=(VMEM, VMEM), compiler_params=params(6), cost_estimate=cost(1), name="pack",
                       )(place, p_low, interp, p_high)
    p_pair, p_other = exchange(pair, other, "slab")
    extent = nx + 2 * REACH
    field = pltpu.VMEM((3, tiles, extent, 3 * SUB, LANES), f32)
    basis, sums = call(
        krylov_kernel,
        out_shape=(shape((3 * ITERS, tiles * nx * ny, LANES), f32), shape((SUB, LANES), f32)),
        in_specs=[SMEM] + [VMEM] * 10,
        out_specs=(VMEM, VMEM),
        scratch_shapes=[pltpu.VMEM((tiles, extent, 3 * SUB, LANES), f32)] * 2 + [field] * 4,
        compiler_params=params(20), cost_estimate=cost(7), name="krylov",
    )(place, interp, p_low, p_high, p_pair, p_other, mixed, from_low, from_high, pair_in, other_in)
    sums = far_hops(sums, "dom")
    sums = far_hops(sums, "slab")
    fields = 3 * ITERS
    short = -(-ways * fields // SUB) * SUB
    kept, message = shape((short, LANES), f32), shape((SUB + short, LANES), f32)
    keep, pair, other = call(
        functools.partial(surface_kernel, nz), out_shape=(kept, message, message), in_specs=[SMEM, SMEM, VMEM, VMEM],
        out_specs=(VMEM,) * 3, scratch_shapes=[pltpu.VMEM((2 * SUB, LANES), i32), pltpu.VMEM((2 * SUB, LANES), f32)],
        compiler_params=params(6), cost_estimate=cost(4), name="surface",
    )(tally, place, basis, boundary.reshape(-1, 1, LANES))
    plain = call(plain_kernel, out_shape=shape((3 * ITERS, nx, ny, nz), f32), in_specs=[VMEM], out_specs=VMEM,
                 compiler_params=params(6), cost_estimate=cost(3), name="plain")(after(basis, pair))
    pair_in, sent, other_in = pair_hops(sums, pair, other, "dom")
    keep, pair, other = call(
        route_kernel, out_shape=(kept, message, message), in_specs=[SMEM] + [VMEM] * 4,
        out_specs=(VMEM,) * 3, compiler_params=params(4), cost_estimate=cost(1), name="route",
    )(place, keep, pair_in, sent, other_in)
    row_hot, lane_hot = call(
        hot_kernel, out_shape=(shape((ways * ways, heat.shape[0], LANES), jnp.bfloat16),
                               shape((ways * ways, LANES, LANES), jnp.bfloat16)),
        in_specs=[VMEM], out_specs=(VMEM, VMEM), compiler_params=params(4), cost_estimate=cost(1), name="hot",
    )(after(accepting, pair).reshape(-1, 1, LANES))
    pair_in = lax.ppermute(pair, "slab", even_odd("slab"))
    sent = lax.dynamic_update_slice(other, pair[:SUB] + pair_in[:SUB], (0, 0))
    other_in = lax.ppermute(sent, "slab", odd_even("slab", True))
    return call(
        finish_kernel,
        out_shape=(shape((3, nx, ny, nz), f32), shape((3, heat_level.shape[0]), f32)),
        in_specs=[SMEM] + [VMEM] * 7,
        out_specs=(HBM, HBM),
        scratch_shapes=[pltpu.VMEM((3, nx, ny, nz), f32), pltpu.VMEM((3, heat_level.shape[0]), f32),
                        pltpu.VMEM(heat.shape, f32), pltpu.SemaphoreType.DMA((3,))],
        compiler_params=params(8), cost_estimate=cost(2), name="finish",
    )(place, keep, pair_in, sent, other_in, plain, row_hot, lane_hot)


def solution(mesh):
    both = ("dom", "slab")
    in_specs = (
        P(both),
        P(both, None, None, None),
        P(None, "dom", "slab", None),
        P(None, "dom", "slab", None),
        P(None, "dom", "slab", None),
        P("dom", "slab", None),
        P(both, None, None, None),
        P(both, None),
        P(both, None, None, None),
    )
    out_specs = (P(None, "dom", "slab", None), P(None, both))

    return jax.shard_map(on_device, mesh=mesh, in_specs=in_specs, out_specs=out_specs, check_vma=False)
```

```python
import functools
import math

import jax
import jax.numpy as jnp
from jax import lax
from jax.experimental import pallas as pl
from jax.experimental.pallas import tpu as pltpu
from jax.sharding import PartitionSpec as P

ITERS = 4
COEF = 0.5
LANES = 128
CHUNK = 16
WEIGHT = 4e8
DEPART_MIB = 56
SUB = 8
CENTRE = 7.125
HALF = 6.875
REACH = ITERS + 1
VMEM = pl.BlockSpec(memory_space=pltpu.VMEM)
SMEM = pl.BlockSpec(memory_space=pltpu.SMEM)
HBM = pl.BlockSpec(memory_space=pltpu.HBM)


def params(mib):
    return pltpu.CompilerParams(vmem_limit_bytes=mib * 1024 * 1024)


def cost(micro, moved=0):
    return pl.CostEstimate(flops=int(micro * WEIGHT), bytes_accessed=moved, transcendentals=0)


def permute(value, lanes):
    return jnp.take_along_axis(value, lanes, axis=1, mode="promise_in_bounds")


def mix(values):
    tiles = len(values)
    lane = lax.broadcasted_iota(jnp.int32, values[0].shape, 1)
    share = LANES // tiles
    mixed = []
    for t in range(tiles):
        source = (lane * tiles + t) % LANES
        total = permute(values[0], source)
        for k in range(1, tiles):
            total = jnp.where(lane >= k * share, permute(values[k], source), total)
        mixed.append(total)
    return mixed


def unmix(values):
    tiles = len(values)
    lane = lax.broadcasted_iota(jnp.int32, values[0].shape, 1)
    share = LANES // tiles
    plain = []
    for k in range(tiles):
        source = k * share + lane // tiles
        total = permute(values[0], source)
        for t in range(1, tiles):
            total = jnp.where(lane % tiles == t, permute(values[t], source), total)
        plain.append(total)
    return plain


def wedge(nx, reach):
    rows, offset = [], 0
    for x in range(1 - reach, nx + reach - 1):
        width = reach - max(0, -x, x - nx + 1)
        rows.append((x, width, offset))
        offset += width
    return rows, offset


def lookup(table, first, rows, lanes, bits):
    if rows == 1:
        row = jnp.broadcast_to(table[pl.ds(first, 1), :], lanes.shape)
        return jnp.take_along_axis(row, lanes, axis=1, mode="promise_in_bounds")
    half = rows // 2
    lower = lookup(table, first, half, lanes, bits[:-1])
    upper = lookup(table, first + half, half, lanes, bits[:-1])
    return jnp.where(bits[-1], upper, lower)


def lookup_all(table, indices, chunk):
    rows = table.shape[0]
    depth = int(math.log2(chunk))
    lanes = [index & (LANES - 1) for index in indices]
    high = [index >> 7 for index in indices]
    outer = [value >> depth for value in high]

    def step(block, found):
        base = pl.multiple_of(block * chunk, chunk)
        fresh = []
        for lane, value, top, old in zip(lanes, high, outer, found):
            bits = [((value >> bit) & 1) == 1 for bit in range(depth)]
            fresh.append(jnp.where(top == block, lookup(table, base, chunk, lane, bits), old))
        return tuple(fresh)

    zero = jnp.zeros(indices[0].shape, jnp.float32)
    return lax.fori_loop(0, rows // chunk, step, tuple(zero for _ in indices))


def order2(a, b):
    if len(a) == 1:
        return (jnp.minimum(a[0], b[0]),), (jnp.maximum(a[0], b[0]),)
    swap = a[0] > b[0]
    low = [jnp.minimum(a[0], b[0])] + [jnp.where(swap, y, x) for x, y in zip(a[1:], b[1:])]
    high = [jnp.maximum(a[0], b[0])] + [jnp.where(swap, x, y) for x, y in zip(a[1:], b[1:])]
    return tuple(low), tuple(high)


def sublane_xor(value, mask):
    sub = lax.broadcasted_iota(jnp.int32, value.shape, 0)
    return jnp.take_along_axis(value, sub ^ mask, axis=0, mode="promise_in_bounds")


def keep_one(a, other, lower):
    if len(a) == 1:
        return (jnp.where(lower, jnp.minimum(a[0], other[0]), jnp.maximum(a[0], other[0])),)
    take = (a[0] > other[0]) == lower
    return tuple(jnp.where(take, y, x) for x, y in zip(a, other))


def sort_rows(refs, block, done=0, until=None):
    count = refs[0].shape[0] // SUB

    def load(v):
        at = pl.ds(pl.multiple_of(v * SUB, SUB), SUB)
        return tuple(r[at, :] for r in refs)

    def store(v, value):
        at = pl.ds(pl.multiple_of(v * SUB, SUB), SUB)
        for r, x in zip(refs, value): r[at, :] = x

    def strides(held, stride):
        while stride:
            for i in range(len(held)):
                if not i & stride:
                    held[i], held[i | stride] = order2(held[i], held[i | stride])
            stride //= 2

    def whole(t, carry):
        held = [load(t * block + i) for i in range(block)]
        size = 2
        while size <= block:
            for i in range(block):
                j = i ^ (size - 1)
                if i < j: held[i], held[j] = order2(held[i], held[j])
            strides(held, size // 4)
            size *= 2
        for i in range(block): store(t * block + i, held[i])
        return carry

    def finish(t, carry):
        held = [load(t * block + i) for i in range(block)]
        strides(held, block // 2)
        for i in range(block): store(t * block + i, held[i])
        return carry

    if not done:
        lax.fori_loop(0, count // block, whole, 0, unroll=2)
    size = 2 * max(done, block)
    while size <= (until or count * SUB):
        span = min(size, count)
        flip = size // count - 1 if size > count else 0
        groups = span // block

        def top(t, carry):
            base = (t // (block // 2)) * span
            i = t % (block // 2)
            spots = []
            for j in range(groups):
                spots += [base + i + block * j, base + block - 1 - i + block * j]
            held = [load(v) for v in spots]
            n = len(held)
            if flip:
                sub = lax.broadcasted_iota(jnp.int32, (SUB, LANES), 0)
                lower = (sub & ((flip + 1) // 2)) == 0
                turned = [tuple(sublane_xor(x, flip) for x in h) for h in held]
                held = [keep_one(held[k], turned[n - 1 - k], lower) for k in range(n)]
                bit = (flip + 1) // 4
                while bit:
                    lower = (sub & bit) == 0
                    held = [keep_one(h, tuple(sublane_xor(x, bit) for x in h), lower) for h in held]
                    bit //= 2
                far = groups // 2
            else:
                for k in range(n // 2):
                    held[k], held[n - 1 - k] = order2(held[k], held[n - 1 - k])
                far = groups // 4
            while far:
                for j in range(groups):
                    if not j & far:
                        for side in range(2):
                            x, y = 2 * j + side, 2 * (j | far) + side
                            held[x], held[y] = order2(held[x], held[y])
                far //= 2
            for v, h in zip(spots, held): store(v, h)
            return carry

        lax.fori_loop(0, (count // span) * (block // 2), top, 0, unroll=max(1, 16 // groups))
        lax.fori_loop(0, count // block, finish, 0, unroll=2)
        size *= 2


def blocks_of(place):
    kinds = 1 + place[0] + place[1]
    return kinds, 1 - place[0], 2 - place[4], 1 + place[4]


def plan_kernel(per, place, shift, bucket, keys):
    kinds, first, left, right = blocks_of(place)
    corners, nx, _, nz = shift.shape
    tiles = nz // LANES
    count = corners * nx * tiles
    sub = lax.broadcasted_iota(jnp.int32, (SUB, LANES), 0)

    def build(x, carry):
        for c in range(corners):
            for t in range(tiles):
                at = pl.ds(t * LANES, LANES)
                way = shift[c, x, :, at]
                a = (way * 11) >> 5
                b = way - 3 * a
                block = jnp.where(b == 1, 0, jnp.where(b == 0, left * kinds, right * kinds)) + (a - first)
                flat = block * (per * LANES) + bucket[c, x, :, at]
                if c:
                    flat = pltpu.roll(flat, c * (LANES // corners), axis=1)
                v = (c * nx + x) * tiles + t
                keys[pl.ds(pl.multiple_of(v * SUB, SUB), SUB), :] = flat * (count * SUB) + (sub * count + v)
        return carry

    lax.fori_loop(0, nx, build, 0, unroll=2)
    sort_rows([keys], 32, until=count)


def order_kernel(per, place, begun, keys, bounds):
    keys[...] = begun[...]
    count = keys.shape[0] // SUB
    sort_rows([keys], 32, done=count)
    low_bits = int(math.log2(count * SUB * LANES))
    lane = lax.broadcasted_iota(jnp.int32, (SUB, LANES), 1)
    base = jnp.zeros((SUB, LANES), jnp.float32)
    width = jnp.zeros((SUB, 1), jnp.float32)
    top = jnp.zeros((SUB, 1), jnp.float32)
    for g in range(count // SUB):
        least = (keys[pl.ds(g * SUB * SUB, SUB), :] >> low_bits).astype(jnp.float32)
        most = (keys[pl.ds(g * SUB * SUB + SUB * (SUB - 1), SUB), :] >> low_bits).astype(jnp.float32)
        least = jnp.min(least, axis=1, keepdims=True)
        most = jnp.max(most, axis=1, keepdims=True)
        base = jnp.where(lane == g, least, base)
        width = jnp.maximum(width, most - least + 1.0)
        top = jnp.maximum(top, most)
    trips = (width.astype(jnp.int32) + (CHUNK - 1)) // CHUNK
    ready = 2 * blocks_of(place)[0] * per
    rows = jnp.where(top.astype(jnp.int32) < ready, ready, 9 * per)
    start = jnp.minimum(base.astype(jnp.int32), rows - trips * CHUNK)
    latest = jnp.max(jnp.where(lane < count // SUB, start, 0).astype(jnp.float32), axis=1, keepdims=True)
    soon = jnp.clip((ready - latest.astype(jnp.int32)) // CHUNK, 0, trips)
    bounds[...] = jnp.where(lane == LANES - 1, trips, jnp.where(lane == LANES - 2, soon, start))


def visit(table, keys, bounds, soon, before, store):
    count = keys.shape[0] // SUB
    pos_bits = int(math.log2(count * SUB))
    per = count // SUB

    def body(s, carry):
        own = [keys[pl.ds(SUB * SUB * g + s, SUB, stride=SUB), :] for g in range(per)]
        start = [bounds[s, g] for g in range(per)]

        def step(offset, chunk, found):
            depth = int(math.log2(chunk))
            fresh = []
            for g in range(per):
                lanes = (own[g] >> pos_bits) & (LANES - 1)
                first = start[g] + offset
                rel = (own[g] >> (pos_bits + 7)) - first
                bits = [((rel >> b) & 1) == 1 for b in range(depth)]
                fresh.append(jnp.where((rel >> depth) == 0, lookup(table, first, chunk, lanes, bits), found[g]))
            return tuple(fresh)

        spots = [pl.ds(SUB * SUB * g + s, SUB, stride=SUB) for g in range(per)]
        least = 0 if soon else bounds[s, LANES - 2]
        most = bounds[s, LANES - 2 if soon else LANES - 1]
        twos = (most - least) // 2
        found = tuple(before(at) for at in spots)
        found = lax.fori_loop(0, twos, lambda n, f: step((least + 2 * n) * CHUNK, 2 * CHUNK, f), found)
        found = lax.fori_loop(least + 2 * twos, most, lambda n, f: step(n * CHUNK, CHUNK, f), found)
        for g, at in enumerate(spots):
            store(at, found[g], own[g] & (count * SUB - 1))
        return carry

    lax.fori_loop(0, SUB, body, 0)


def slots_of(heat, picks, first, out, rows):
    group = SUB * SUB

    def body(g, carry):
        base = pl.multiple_of(g * group, group)
        found = lookup_all(heat, [picks[pl.ds(first + base + SUB * k, SUB), :] for k in range(SUB)], heat.shape[0])
        for k in range(SUB):
            out[pl.ds(base + SUB * k, SUB), :] = found[k]
        return carry

    lax.fori_loop(0, rows // group, body, 0, unroll=True)


def depart_kernel(heat_hbm, picks_hbm, rigid_hbm, up, heat, picks, rigid, arrived):
    rows, narrow = picks.shape[0], rigid.shape[0]
    sources = (rigid_hbm.at[pl.ds(rigid_hbm.shape[0] - narrow, narrow)], heat_hbm,
               picks_hbm.at[pl.ds(picks_hbm.shape[0] - rows, rows), :])
    copies = [
        pltpu.make_async_copy(source, target, arrived.at[k])
        for k, (source, target) in enumerate(zip(sources, (rigid, heat, picks)))
    ]
    for copy in copies:
        copy.start()
    tiles = rigid.shape[2] // LANES
    copies[0].wait()
    for x in range(narrow):
        for t, value in enumerate(mix([rigid[x, :, pl.ds(t * LANES, LANES)] for t in range(tiles)])):
            up[pl.ds(rows + (x * tiles + t) * SUB, SUB), :] = value
    copies[1].wait()
    copies[2].wait()
    slots_of(heat, picks, 0, up, rows)


def depart_down_kernel(heat, picks, rigid, down, mixed):
    narrow = REACH - 2
    nx, _, nz = rigid.shape
    tiles = nz // LANES
    rows = down.shape[0] - narrow * tiles * SUB
    for x in range(nx):
        for t, value in enumerate(mix([rigid[x, :, pl.ds(t * LANES, LANES)] for t in range(tiles)])):
            mixed[x, pl.ds(t * SUB, SUB), :] = value
            if x < narrow:
                down[pl.ds(rows + (x * tiles + t) * SUB, SUB), :] = value
    slots_of(heat, picks, 0, down, rows)


def near_kernel(heat, picks, near):
    slots_of(heat, picks, near.shape[0], near, near.shape[0])


def forward_kernel(place, low, near, high, rigid, pair, other):
    nx, ny = rigid.shape[0], SUB
    per = near.shape[0] // 3
    tiles = rigid.shape[1] // SUB
    odd = place[4] == 1
    rows, size = wedge(nx, REACH - 2)

    def give(to, up, down):
        pair[to, :] = jnp.where(odd, down, up)
        other[to, :] = jnp.where(odd, up, down)

    for a, ref in enumerate((low, near, high)):
        give(pl.ds(a * per, per), ref[pl.ds(2 * per, per), :], ref[pl.ds(0, per), :])
    for t in range(tiles):
        for x, width, offset in rows:
            to = pl.ds(3 * per + t * size + offset, width)
            if 0 <= x < nx:
                base = t * SUB
                give(to, rigid[x, pl.ds(base + ny - width, width), :], rigid[x, pl.ds(base, width), :])
            else:
                ref, k = (low, x + REACH - 2) if x < 0 else (high, x - nx)
                base = 3 * per + (k * tiles + t) * SUB
                give(to, ref[pl.ds(base + ny - width, width), :], ref[pl.ds(base, width), :])


def lay(table, per, place, columns):
    kinds, first = blocks_of(place)[:2]
    for valid, column, readers in columns:
        for a, read in enumerate(readers):
            here = valid if a == 1 else jnp.logical_and(valid, place[0 if a == 0 else 1] == 1)

            @pl.when(here)
            def _():
                row = pl.multiple_of((column * kinds + a - first) * per, per)
                table[pl.ds(row, per), :] = read()


def early_kernel(place, pair, low, near, high, keys, bounds, value, table):
    per = near.shape[0] // 3
    own = [lambda ref=ref: ref[pl.ds(per, per), :] for ref in (low, near, high)]
    side = [lambda at=pl.ds(a * per, per): pair[at, :] for a in range(3)]
    lay(table, per, place, [(place[0] >= 0, 0, own), (place[0] >= 0, 1, side)])

    def store(at, found, spot):
        value[at, :] = found

    visit(table, keys, bounds, True, lambda at: jnp.zeros((SUB, LANES), jnp.float32), store)


def pick_kernel(place, pair, other, low, near, high, keys, early, bounds, factor, out, table, position, value):
    odd = place[4] == 1
    corners, nx, _, nz = factor.shape
    tiles = nz // LANES
    slots = near.shape[0] // 3
    own = [lambda ref=ref: ref[pl.ds(slots, slots), :] for ref in (low, near, high)]

    def side(even_ref, odd_ref):
        return [lambda at=pl.ds(a * slots, slots): jnp.where(odd, odd_ref[at, :], even_ref[at, :]) for a in range(3)]

    _, _, left, right = blocks_of(place)
    lay(table, slots, place, [(place[0] >= 0, 0, own), (place[2] == 1, left, side(other, pair)),
                              (place[3] == 1, right, side(pair, other))])

    def store(at, found, spot):
        value[at, :] = found
        position[at, :] = spot

    visit(table, keys, bounds, False, lambda at: early[at, :], store)
    sort_rows([position, value], 16)

    def blend(x, carry):
        blended = []
        for t in range(tiles):
            at = pl.ds(t * LANES, LANES)
            total = None
            for c in range(corners):
                v = (c * nx + x) * tiles + t
                got = value[pl.ds(pl.multiple_of(v * SUB, SUB), SUB), :]
                if c:
                    got = pltpu.roll(got, LANES - c * (LANES // corners), axis=1)
                got = factor[c, x, :, at] * got
                total = got if total is None else total + got
            blended.append(total)
        for t, total in enumerate(mix(blended)):
            out[x, pl.ds(t * SUB, SUB), :] = total
        return carry

    lax.fori_loop(0, nx, blend, 0, unroll=2)


def pack_kernel(place, low, own, high, pair, other):
    nx, ny = own.shape[0], SUB
    tiles = own.shape[1] // SUB
    odd = place[4] == 1
    rows, size = wedge(nx, REACH)
    for t in range(tiles):
        for x, width, offset in rows:
            ref, k = (own, x) if 0 <= x < nx else (low, x + REACH) if x < 0 else (high, x - nx)
            up = ref[k, pl.ds(t * SUB + ny - width, width), :]
            down = ref[k, pl.ds(t * SUB, width), :]
            to = pl.ds(t * size + offset, width)
            pair[to, :] = jnp.where(odd, down, up)
            other[to, :] = jnp.where(odd, up, down)


def unpack(target, reach, own, dom_low, dom_high, pair, other, offset, odd, change):
    nx = own.shape[0]
    tiles = own.shape[1] // SUB
    rows, size = wedge(nx, reach)
    for t in range(tiles):
        for x in range(-reach, nx + reach):
            if 0 <= x < nx:
                mine = own[x, pl.ds(t * SUB, SUB), :]
            else:
                mine = dom_low(x + reach, t) if x < 0 else dom_high(x - nx, t)
            target[t, REACH + x, pl.ds(SUB, SUB), :] = change(mine, REACH + x, 1)
        for x, width, row in rows:
            at = pl.ds(offset + t * size + row, width)
            even_low, odd_low = other[at, :], pair[at, :]
            target[t, REACH + x, pl.ds(SUB - width, width), :] = change(jnp.where(odd, odd_low, even_low), REACH + x, 0)
            target[t, REACH + x, pl.ds(2 * SUB, width), :] = change(jnp.where(odd, even_low, odd_low), REACH + x, 2)


def krylov_kernel(inside, own, p_low, p_high, p_pair, p_other, rigid, d_low, d_high, d_pair, d_other,
                  basis, sums, temp, diag, u0, u1, u2, u3):
    nx = own.shape[0]
    tiles = own.shape[1] // SUB
    parts = temp.shape[2] // SUB
    held = (u0, u1, u2, u3)
    flag = [inside[k].astype(jnp.float32) for k in range(4)]

    def mask(x, part):
        at_x = jnp.where(x < REACH, flag[0], jnp.where(x >= REACH + nx, flag[1], 1.0))
        return at_x * (flag[2] if part == 0 else flag[3] if part == 2 else 1.0)

    temp[...] = jnp.zeros_like(temp)
    odd = inside[4] == 1
    base = d_pair.shape[0] - tiles * wedge(nx, REACH - 2)[1]
    first_d = d_low.shape[0] - tiles * SUB * (REACH - 2)

    def plane(ref):
        return lambda x, t: ref[x, pl.ds(t * SUB, SUB), :]

    def message(ref):
        return lambda x, t: ref[pl.ds(first_d + (x * tiles + t) * SUB, SUB), :]

    unpack(temp, REACH, own, plane(p_low), plane(p_high), p_pair, p_other, 0, odd, lambda v, x, part: v)
    diag[...] = jnp.zeros_like(diag)
    unpack(diag, REACH - 2, rigid, message(d_low), message(d_high), d_pair, d_other, base, odd,
           lambda v, x, part: (v * (2.0 / HALF) + 2.0 * (6.0 - CENTRE) / HALF) * mask(x, part))
    lane = lax.broadcasted_iota(jnp.int32, (SUB, LANES), 1)
    first, last = lane == 0, lane == LANES - 1
    zero = jnp.zeros((SUB, LANES), jnp.float32)

    def around_z(values):
        back = jnp.where(first, zero, pltpu.roll(values[-1], 1, axis=1))
        ahead = jnp.where(last, zero, pltpu.roll(values[0], LANES - 1, axis=1))
        return [(values[t - 1] if t else back, values[t + 1] if t + 1 < tiles else ahead) for t in range(tiles)]

    def around_y(ref, head, x, part):
        base = part * SUB
        mine = ref[(*head, x, pl.ds(base, SUB))]
        below = pltpu.roll(mine, 1, axis=0) if part == 0 else ref[(*head, x, pl.ds(base - 1, SUB))]
        above = pltpu.roll(mine, SUB - 1, axis=0) if part == parts - 1 else ref[(*head, x, pl.ds(base + 1, SUB))]
        return mine, below, above

    def load_row(x, carry):
        for part in range(parts):
            scale = COEF * mask(x, part)
            rows = [around_y(temp, (t,), x, part) for t in range(tiles)]
            along = around_z([r[0] for r in rows])
            for t in range(tiles):
                ahead = temp[t, x + 1, pl.ds(part * SUB, SUB), :]
                back = temp[t, x - 1, pl.ds(part * SUB, SUB), :]
                u0[0, t, x, pl.ds(part * SUB, SUB), :] = scale * (ahead - back)
                u0[1, t, x, pl.ds(part * SUB, SUB), :] = scale * (rows[t][2] - rows[t][1])
                u0[2, t, x, pl.ds(part * SUB, SUB), :] = scale * (along[t][1] - along[t][0])
        return carry

    lax.fori_loop(1, nx + 2 * REACH - 1, load_row, 0, unroll=4 if nx == SUB else 1)

    def twice(ref, c, x, part):
        coefficient = (2.0 / HALF) * mask(x, part)
        rows = [around_y(ref, (c, t), x, part) for t in range(tiles)]
        along = around_z([r[0] for r in rows])
        results = []
        for t in range(tiles):
            near = rows[t][1] + rows[t][2] + along[t][0] + along[t][1]
            near = near + ref[c, t, x + 1, pl.ds(part * SUB, SUB), :] + ref[c, t, x - 1, pl.ds(part * SUB, SUB), :]
            results.append(diag[t, x, pl.ds(part * SUB, SUB), :] * rows[t][0] - coefficient * near)
        return results, [r[0] for r in rows]

    for order in range(1, ITERS):
        source, target = held[order - 1], held[order]

        def apply_row(x, carry):
            for c in range(3):
                for part in range(parts):
                    doubled, _ = twice(source, c, x, part)
                    for t in range(tiles):
                        at = (c, t, x, pl.ds(part * SUB, SUB))
                        if order == 1:
                            target[at] = 0.5 * doubled[t]
                        else:
                            target[at] = doubled[t] - held[order - 2][at]
            return carry

        margin = ITERS - order
        lax.fori_loop(REACH - margin, REACH + nx + margin, apply_row, 0, unroll=(2, 4, 5)[order - 1] if nx == SUB else 1)

    def dots_row(x, carry):
        carry = list(carry)
        for c in range(3):
            doubled, u = twice(u3, c, REACH + x, 1)
            for t in range(tiles):
                at = (c, t, REACH + x, pl.ds(SUB, SUB))
                v = [u0[at], u1[at], u2[at], u[t]]
                pairs = [(v[0], v[0]), (v[0], v[1]), (v[1], v[1]), (v[1], v[2]), (v[2], v[2]), (v[2], v[3]),
                         (v[3], v[3]), (v[3], doubled[t])]
                for k, (left, right) in enumerate(pairs):
                    carry[k] = carry[k] + left * right
                for j in range(4):
                    basis[3 * j + c, pl.ds(pl.multiple_of(t * nx * SUB + x * SUB, SUB), SUB), :] = v[j]
        return tuple(carry)

    totals = lax.fori_loop(0, nx, dots_row, tuple(zero for _ in range(8)), unroll=4 if nx == SUB else 1)
    for k in range(8):
        sums[pl.ds(k, 1), :] = jnp.sum(totals[k], axis=0, keepdims=True)


def surface_kernel(nz, tally, place, basis, picks, keep, pair, other, index, live):
    fields, rows, _ = basis.shape
    count = picks.shape[0]
    tiles = nz // LANES
    block = rows // tiles
    odd = place[6] == 1
    lane = lax.broadcasted_iota(jnp.int32, (1, LANES), 1)
    sub = lax.broadcasted_iota(jnp.int32, (SUB, LANES), 0)
    for k in range(count):
        spot = picks[k]
        along = spot % nz
        index[pl.ds(k, 1), :] = ((along % tiles) * block + spot // nz) * LANES + along // tiles
        live[pl.ds(k, 1), :] = (lane < tally[0, k]).astype(jnp.float32)

    def give(f, values):
        for b in range(3):
            keep[pl.ds(b * fields + f, 1), :] = values[3 + b]
            to = pl.ds(SUB + b * fields + f, 1)
            pair[to, :] = jnp.where(odd, values[b], values[6 + b])
            other[to, :] = jnp.where(odd, values[6 + b], values[b])

    depth = int(math.log2(rows))

    def body(f, carry):
        table = basis.at[f]
        spots = index[pl.ds(0, SUB), :]
        high = spots >> 7
        bits = [((high >> bit) & 1) == 1 for bit in range(depth)]
        found = lookup(table, 0, rows, spots & (LANES - 1), bits)
        found = jnp.where(live[pl.ds(0, SUB), :] > 0.5, found, 0.0)
        values = [found[k : k + 1, :] for k in range(SUB)]
        for k in range(SUB, count):
            spots = jnp.broadcast_to(index[pl.ds(k, 1), :], (SUB, LANES))
            lanes, high = spots & (LANES - 1), spots >> 7
            total = jnp.zeros((SUB, LANES), jnp.float32)
            for g in range(0, rows, SUB):
                got = jnp.take_along_axis(table[pl.ds(g, SUB), :], lanes, axis=1, mode="promise_in_bounds")
                total = jnp.where(high == sub + g, got, total)
            total = jnp.sum(total, axis=0, keepdims=True)
            total = jnp.where(live[pl.ds(k, 1), :] > 0.5, total, 0.0)
            values.append(total)
        give(f, values)
        return carry

    lax.fori_loop(0, fields, body, 0, unroll=4)


def route_kernel(place, kept, pair_in, sent, other_in, keep, pair, other):
    fields = 3 * ITERS
    pair[pl.ds(0, SUB), :] = sent[pl.ds(0, SUB), :] + other_in[pl.ds(0, SUB), :]
    odd, odd_dom = place[4] == 1, place[6] == 1
    for b in range(3):
        at = pl.ds(SUB + b * fields, fields)
        one, two = pair_in[at, :], other_in[at, :]
        low = jnp.where(odd_dom, one, two) * place[0].astype(jnp.float32)
        high = jnp.where(odd_dom, two, one) * place[1].astype(jnp.float32)
        for a, rows in ((0, low), (1, kept[pl.ds(b * fields, fields), :]), (2, high)):
            if b == 1:
                keep[pl.ds(a * fields, fields), :] = rows
            else:
                to = pl.ds(SUB + a * fields, fields)
                chosen = odd if b == 0 else jnp.logical_not(odd)

                @pl.when(chosen)
                def _():
                    pair[to, :] = rows

                @pl.when(jnp.logical_not(chosen))
                def _():
                    other[to, :] = rows


def coefficients(nu):
    half = 0.5

    def gram(i, j):
        return half * (nu[i + j] + nu[abs(i - j)])

    def inner(i, j):
        if j == 0:
            return gram(i, 1)
        return half * (gram(i, j + 1) + gram(i, j - 1))

    def form(vector, matrix):
        n = len(vector)
        total = None
        for i in range(n):
            for j in range(i, n):
                term = vector[i] * vector[j] * matrix(i, j)
                term = term if i == j else 2.0 * term
                total = term if total is None else total + term
        return total

    one = jnp.ones_like(nu[0])
    found, residual, direction = [], [one], [one]
    rr = nu[0]
    for iteration in range(ITERS):
        energy = form(direction, lambda i, j: CENTRE * gram(i, j) + HALF * inner(i, j))
        alpha = rr / energy
        found = [
            (found[i] if i < len(found) else 0.0) + alpha * direction[i] for i in range(len(direction))
        ]
        if iteration + 1 == ITERS:
            break
        image = [CENTRE * d for d in direction] + [jnp.zeros_like(one)]
        for j, d in enumerate(direction):
            if j == 0:
                image[1] = image[1] + HALF * d
            else:
                image[j + 1] = image[j + 1] + half * HALF * d
                image[j - 1] = image[j - 1] + half * HALF * d
        residual = residual + [jnp.zeros_like(one)]
        residual = [r - alpha * w for r, w in zip(residual, image)]
        fresh = form(residual, gram)
        ratio = fresh / rr
        direction = direction + [jnp.zeros_like(one)]
        direction = [r + ratio * d for r, d in zip(residual, direction)]
        rr = fresh
    return found


def plain_kernel(basis, plain):
    fields, nx, _, nz = plain.shape
    tiles = nz // LANES

    def row(x, carry):
        for f in range(fields):
            at = [pl.ds(pl.multiple_of(t * nx * SUB + x * SUB, SUB), SUB) for t in range(tiles)]
            for t, value in enumerate(unmix([basis[f, k, :] for k in at])):
                plain[f, x, :, pl.ds(t * LANES, LANES)] = value
        return carry

    lax.fori_loop(0, nx, row, 0, unroll=2)


def hot_kernel(picks, row_hot, lane_hot):
    count = picks.shape[0]
    place = lax.broadcasted_iota(jnp.int32, lane_hot.shape[1:], 0)
    tall = lax.broadcasted_iota(jnp.int32, row_hot.shape[1:], 0)
    for k in range(count):
        spot = picks[k]
        lane_hot[k] = (place == spot % LANES).astype(jnp.float32).astype(jnp.bfloat16)
        row_hot[k] = (tall == spot // LANES).astype(jnp.float32).astype(jnp.bfloat16)


def finish_kernel(place, keep, pair, sent, other, basis, row_hot, lane_hot, disp_hbm, thermal_hbm, disp, thermal, shift,
                  left):
    sums = sent[pl.ds(0, SUB), :] + other[pl.ds(0, SUB), :]
    raw = [jnp.broadcast_to(jnp.sum(sums[k : k + 1, :], axis=1, keepdims=True), (1, LANES)) for k in range(8)]
    nu = [raw[0], raw[1]]
    for k in range(2, 7):
        nu.append(2.0 * raw[k] - raw[k % 2])
    nu.append(2.0 * raw[7] - nu[5] - 2.0 * raw[1])
    weights = coefficients(nu)
    wide = [jnp.broadcast_to(w, (SUB, LANES)) for w in weights]
    _, nx, _, nz = disp.shape
    tiles = nz // LANES
    depth = thermal.shape[1] // LANES
    fields = 3 * ITERS
    total = jnp.zeros((9 * depth, LANES), jnp.float32)
    odd = place[4]
    blocks = []
    for ref, offset, b, here in (
        (keep, 0, 1, 1),
        (pair, SUB, 2 - 2 * odd, jnp.where(odd == 1, place[2], place[3])),
        (other, SUB, 2 * odd, jnp.where(odd == 1, place[3], place[2])),
    ):
        valid = jnp.full((1, LANES), here, jnp.int32) == 1
        for a in range(3):
            pieces = []
            for c in range(3):
                value = None
                for j in range(ITERS):
                    term = weights[j] * ref[pl.ds(offset + a * fields + 3 * j + c, 1), :]
                    value = term if value is None else value + term
                value = jnp.where(valid, value, 0.0)
                for _ in range(3):
                    part = value.astype(jnp.bfloat16)
                    value = value - part.astype(jnp.float32)
                    pieces.append(row_hot[3 * a + b] * jnp.broadcast_to(part, (depth, LANES)))
            blocks.append((jnp.concatenate(pieces, axis=0), lane_hot[3 * a + b]))
            if len(blocks) == 2 or (ref is other and a == 2):
                wanted = jnp.concatenate([p for p, _ in blocks], axis=1)
                hot = jnp.concatenate([h for _, h in blocks], axis=1)
                total = total + lax.dot_general(wanted, hot, (((1,), (1,)), ((), ())),
                                                preferred_element_type=jnp.float32)
                blocks = []
    for c in range(3):
        whole = total[3 * c * depth : (3 * c + 1) * depth]
        whole = whole + total[(3 * c + 1) * depth : (3 * c + 2) * depth]
        shift[...] = whole + total[(3 * c + 2) * depth : (3 * c + 3) * depth]
        for r in range(depth):
            thermal[pl.ds(c, 1), pl.ds(r * LANES, LANES)] = shift[pl.ds(r, 1), :]
    copies = [pltpu.make_async_copy(thermal, thermal_hbm, left.at[0])]
    copies[0].start()

    def row(x, carry):
        for c in range(3):
            for t in range(tiles):
                at = pl.ds(t * LANES, LANES)
                total = wide[0] * basis[c, x, :, at]
                for j in range(1, 4):
                    total = total + wide[j] * basis[3 * j + c, x, :, at]
                disp[c, x, :, at] = total
        return carry

    half = nx // 2
    for k in range(2):
        at = pl.ds(k * half, half)
        lax.fori_loop(k * half, (k + 1) * half, row, 0, unroll=2)
        copies.append(pltpu.make_async_copy(disp.at[:, at], disp_hbm.at[:, at], left.at[1 + k]))
        copies[-1].start()
    for copy in copies:
        copy.wait()


def swap(last, leading, axis):
    peers = lax.axis_size(axis)
    up = [(i, i + 1) for i in range(peers - 1)]
    down = [(j, i) for i, j in up]
    return lax.ppermute(last, axis, up), lax.ppermute(leading, axis, down)


def after(value, *others):
    return lax.optimization_barrier((value, *others))[0]


def even_odd(axis):
    return [(i, i ^ 1) for i in range(lax.axis_size(axis))]


def odd_even(axis, around):
    peers = lax.axis_size(axis)
    pairs = [(i, i + 1 if i % 2 else i - 1) for i in range(peers)]
    return [(i, j % peers) for i, j in pairs if around or 0 <= j < peers]


def exchange(pair, other, axis):
    return lax.ppermute(pair, axis, even_odd(axis)), lax.ppermute(other, axis, odd_even(axis, False))


def far_hops(sums, axis):
    peers = lax.axis_size(axis)
    hop = peers // 2
    while hop >= 4:
        sums = sums + lax.ppermute(sums, axis, [(i, (i + hop) % peers) for i in range(peers)])
        hop //= 2
    return sums


def pair_hops(sums, pair, other, axis):
    pair = pair if sums is None else lax.dynamic_update_slice(pair, sums, (0, 0))
    pair_in = lax.ppermute(pair, axis, even_odd(axis))
    sent = lax.dynamic_update_slice(other, pair[:SUB] + pair_in[:SUB], (0, 0))
    other_in = lax.ppermute(sent, axis, odd_even(axis, True))
    return pair_in, sent, other_in


def on_device(heat_level, emitting, holder, bucket, factors, rigidity, boundary, tally, accepting):
    f32, i32 = jnp.float32, jnp.int32
    ways = emitting.shape[1]
    per = emitting.shape[3] // LANES
    nx, ny, nz = rigidity.shape
    tiles = nz // LANES
    narrow = REACH - 2
    call = pl.pallas_call
    shape = jax.ShapeDtypeStruct
    dom, slab = lax.axis_index("dom"), lax.axis_index("slab")
    place = jnp.stack([dom > 0, dom < lax.axis_size("dom") - 1, slab > 0, slab < lax.axis_size("slab") - 1,
                       slab % 2, dom, dom % 2]).astype(i32)
    heat = heat_level.reshape(-1, LANES)
    emit_rows = emitting.reshape(-1, LANES)
    dom_message = shape((ways * per + narrow * tiles * ny, LANES), f32)
    third = shape((ways * per, LANES), i32)
    up = call(
        depart_kernel, out_shape=dom_message, in_specs=[HBM] * 3, out_specs=VMEM,
        scratch_shapes=[pltpu.VMEM(heat.shape, f32), pltpu.VMEM(third.shape, i32), pltpu.VMEM((narrow, ny, nz), f32),
                        pltpu.SemaphoreType.DMA((3,))],
        compiler_params=params(DEPART_MIB), cost_estimate=cost(5), name="depart",
    )(heat, emit_rows, rigidity)
    pairs_up = [(i, i + 1) for i in range(lax.axis_size("dom") - 1)]
    from_low = lax.ppermute(up, "dom", pairs_up)
    down, mixed = call(
        depart_down_kernel, out_shape=(dom_message, shape((nx, tiles * ny, LANES), f32)), in_specs=[VMEM] * 3,
        out_specs=(VMEM,) * 2, compiler_params=params(4), cost_estimate=cost(4), name="down",
    )(after(heat, up), emit_rows, rigidity)
    from_high = lax.ppermute(down, "dom", [(j, i) for i, j in pairs_up])
    near = call(near_kernel, out_shape=shape((ways * per, LANES), f32), in_specs=[VMEM] * 2, out_specs=VMEM,
                compiler_params=params(4), cost_estimate=cost(4), name="near")(after(heat, down), emit_rows)
    count = holder.size // LANES
    rows = ways * ways * per
    begun = call(
        functools.partial(plan_kernel, per), out_shape=shape((count, LANES), i32), in_specs=[SMEM, VMEM, VMEM],
        out_specs=VMEM,
        compiler_params=params(6), cost_estimate=cost(3), name="plan",
    )(place, after(holder, near), bucket)
    slab_message = shape((ways * per + tiles * wedge(nx, narrow)[1], LANES), f32)
    pair, other = call(
        forward_kernel, out_shape=(slab_message,) * 2, in_specs=[SMEM] + [VMEM] * 4, out_specs=(VMEM,) * 2,
        compiler_params=params(6), cost_estimate=cost(1), name="forward",
    )(place, from_low, after(near, begun), from_high, mixed)
    pair_in = lax.ppermute(pair, "slab", even_odd("slab"))
    keys, bounds = call(
        functools.partial(order_kernel, per), out_shape=(shape((count, LANES), i32), shape((SUB, LANES), i32)),
        in_specs=[SMEM, VMEM], out_specs=(VMEM, VMEM), compiler_params=params(6), cost_estimate=cost(3), name="order",
    )(place, after(begun, pair))
    other = after(other, keys, pair_in)
    other_in = lax.ppermute(other, "slab", odd_even("slab", False))
    early = call(
        early_kernel, out_shape=shape((count, LANES), f32), in_specs=[SMEM] + [VMEM] * 5 + [SMEM], out_specs=VMEM,
        scratch_shapes=[pltpu.VMEM((2 * ways * per, LANES), f32)], compiler_params=params(6), cost_estimate=cost(3),
        name="early",
    )(place, pair_in, from_low, near, from_high, keys, bounds)
    interp = call(
        pick_kernel, out_shape=shape((nx, tiles * ny, LANES), f32), in_specs=[SMEM] + [VMEM] * 7 + [SMEM, VMEM],
        out_specs=VMEM,
        scratch_shapes=[pltpu.VMEM((rows, LANES), f32), pltpu.VMEM((count, LANES), i32), pltpu.VMEM((count, LANES), f32)],
        compiler_params=params(8), cost_estimate=cost(12), name="pick",
    )(place, pair_in, other_in, from_low, near, from_high, keys, early, bounds, factors)
    p_low, p_high = swap(interp[nx - REACH :], interp[:REACH], "dom")
    halo = shape((tiles * wedge(nx, REACH)[1], LANES), f32)
    pair, other = call(pack_kernel, out_shape=(halo, halo), in_specs=[SMEM] + [VMEM] * 3,
                       out_specs=(VMEM, VMEM), compiler_params=params(6), cost_estimate=cost(1), name="pack",
                       )(place, p_low, interp, p_high)
    p_pair, p_other = exchange(pair, other, "slab")
    extent = nx + 2 * REACH
    field = pltpu.VMEM((3, tiles, extent, 3 * SUB, LANES), f32)
    basis, sums = call(
        krylov_kernel,
        out_shape=(shape((3 * ITERS, tiles * nx * ny, LANES), f32), shape((SUB, LANES), f32)),
        in_specs=[SMEM] + [VMEM] * 10,
        out_specs=(VMEM, VMEM),
        scratch_shapes=[pltpu.VMEM((tiles, extent, 3 * SUB, LANES), f32)] * 2 + [field] * 4,
        compiler_params=params(20), cost_estimate=cost(7), name="krylov",
    )(place, interp, p_low, p_high, p_pair, p_other, mixed, from_low, from_high, pair_in, other_in)
    sums = far_hops(sums, "dom")
    sums = far_hops(sums, "slab")
    fields = 3 * ITERS
    short = -(-ways * fields // SUB) * SUB
    kept, message = shape((short, LANES), f32), shape((SUB + short, LANES), f32)
    keep, pair, other = call(
        functools.partial(surface_kernel, nz), out_shape=(kept, message, message), in_specs=[SMEM, SMEM, VMEM, VMEM],
        out_specs=(VMEM,) * 3, scratch_shapes=[pltpu.VMEM((2 * SUB, LANES), i32), pltpu.VMEM((2 * SUB, LANES), f32)],
        compiler_params=params(6), cost_estimate=cost(4), name="surface",
    )(tally, place, basis, boundary.reshape(-1, 1, LANES))
    plain = call(plain_kernel, out_shape=shape((3 * ITERS, nx, ny, nz), f32), in_specs=[VMEM], out_specs=VMEM,
                 compiler_params=params(6), cost_estimate=cost(3), name="plain")(after(basis, pair))
    pair_in, sent, other_in = pair_hops(sums, pair, other, "dom")
    keep, pair, other = call(
        route_kernel, out_shape=(kept, message, message), in_specs=[SMEM] + [VMEM] * 4,
        out_specs=(VMEM,) * 3, compiler_params=params(4), cost_estimate=cost(1), name="route",
    )(place, keep, pair_in, sent, other_in)
    row_hot, lane_hot = call(
        hot_kernel, out_shape=(shape((ways * ways, heat.shape[0], LANES), jnp.bfloat16),
                               shape((ways * ways, LANES, LANES), jnp.bfloat16)),
        in_specs=[VMEM], out_specs=(VMEM, VMEM), compiler_params=params(4), cost_estimate=cost(1), name="hot",
    )(after(accepting, pair).reshape(-1, 1, LANES))
    pair_in = lax.ppermute(pair, "slab", even_odd("slab"))
    sent = lax.dynamic_update_slice(other, pair[:SUB] + pair_in[:SUB], (0, 0))
    other_in = lax.ppermute(sent, "slab", odd_even("slab", True))
    return call(
        finish_kernel,
        out_shape=(shape((3, nx, ny, nz), f32), shape((3, heat_level.shape[0]), f32)),
        in_specs=[SMEM] + [VMEM] * 7,
        out_specs=(HBM, HBM),
        scratch_shapes=[pltpu.VMEM((3, nx, ny, nz), f32), pltpu.VMEM((3, heat_level.shape[0]), f32),
                        pltpu.VMEM(heat.shape, f32), pltpu.SemaphoreType.DMA((3,))],
        compiler_params=params(8), cost_estimate=cost(2), name="finish",
    )(place, keep, pair_in, sent, other_in, plain, row_hot, lane_hot)


def solution(mesh):
    both = ("dom", "slab")
    in_specs = (
        P(both),
        P(both, None, None, None),
        P(None, "dom", "slab", None),
        P(None, "dom", "slab", None),
        P(None, "dom", "slab", None),
        P("dom", "slab", None),
        P(both, None, None, None),
        P(both, None),
        P(both, None, None, None),
    )
    out_specs = (P(None, "dom", "slab", None), P(None, both))

    return jax.shard_map(on_device, mesh=mesh, in_specs=in_specs, out_specs=out_specs, check_vma=False)
```
